32 devices in a mesh: tok: 4 (over z), out: 4 (over x, core), grp: 2 (over y).
Axes of the slice: x: 2, y: 2, z: 4, core: 2. Of those that a mesh axis runs over, the one named last changes fastest.
Arguments:
- activations: bfloat16 [1024, 2, 2048], P(('tok', 'grp'), None, 'out'), may hold values from -16 to 16
- out_grads: bfloat16 [1024, 2, 2048], P(('tok', 'grp'), None, 'out'), may hold values from -16 to 16
- weight: bfloat16 [2, 2048, 4096], P(None, 'out'), may hold values from -0.09375 to 0.09375
Outputs:
- update: bfloat16 [4096, 2, 2048], P(('tok', 'grp'), None, 'out')
- input_grad: bfloat16 [1024, 2, 2048], P(('tok', 'grp'), None, 'out')
The draws below stay inside these ranges and needn't reach their ends.
All inputs are finite; a program needn't handle non-finite values.
Results may differ from the reference program's by a relative error of at most 0.0092.
Values may be sent and summed in bfloat16 or wider, within the bound.
A program may use at most 64 MiB of HBM per device.

```python
import math
import jax
import jax.numpy as jnp
from jax import lax

BLOCK = 2048
NBLOCKS = 2
POWER = 3
D = 4096
TOKENS = 1024


def shaped_sides(key):
    noise_key, level_key, reach_key, sign_key, turn_key, weight_key, factor_key = jax.random.split(key, 7)
    array_shape = (TOKENS, NBLOCKS, BLOCK)
    bulk_noise = jnp.clip(jax.random.normal(noise_key, array_shape, jnp.float32), -4.0, 4.0)
    strength = jax.random.uniform(factor_key, (NBLOCKS,), jnp.float32, 1.8, 3.0)
    levels = jnp.exp(jax.random.uniform(level_key, (NBLOCKS, BLOCK), jnp.float32, -1.2, 1.2))
    block_reach = jax.random.uniform(reach_key, (NBLOCKS,), jnp.float32, 0.35, 0.7)
    parity = jnp.where(jnp.arange(NBLOCKS) % 2 == 0, 1.0, -1.0)
    block_sign = jnp.where(jax.random.bernoulli(sign_key, 0.5), 1.0, -1.0)
    magnitude = jnp.exp(block_reach * parity * block_sign)
    squares = levels * levels
    orthonormal = []
    for column_vec in (jnp.ones_like(squares), squares, squares * squares):
        for member in orthonormal:
            column_vec = column_vec - jnp.sum(column_vec * member, axis=1, keepdims=True) * member
        orthonormal.append(column_vec / jnp.sqrt(jnp.sum(column_vec * column_vec, axis=1, keepdims=True)))
    direction = jax.random.normal(turn_key, (NBLOCKS, BLOCK), jnp.float32)
    for member in orthonormal:
        direction = direction - jnp.sum(direction * member, axis=1, keepdims=True) * member
    direction = direction / jnp.sqrt(jnp.sum(direction * direction, axis=1, keepdims=True))
    amplitude = jnp.sqrt(strength * 3.0 * jnp.max(squares, axis=1))
    weights = jax.random.normal(weight_key, (TOKENS, NBLOCKS), jnp.float32)
    shaped = magnitude[None, :, None] * (levels[None] * bulk_noise + amplitude[None, :, None] * weights[:, :, None] * direction[None])
    return jnp.clip(shaped, -16.0, 16.0)


def draw_activations(key, part):
    return shaped_sides(jax.random.fold_in(key, 11)).astype(jnp.bfloat16)


def draw_out_grads(key, part):
    return shaped_sides(jax.random.fold_in(key, 23)).astype(jnp.bfloat16)


def shard_levels(rng, extent, shards, low, largest):
    def one(axis_at, blocks):
        steps = jax.random.uniform(jax.random.fold_in(jax.random.fold_in(rng, 6), axis_at), (blocks,), jnp.float32, low / len(shards), largest / len(shards))
        return jnp.repeat(jnp.exp(steps), extent[axis_at] // blocks).reshape((-1,) + (1,) * (len(extent) - axis_at - 1))

    factor_of = one(*shards[0])
    for cut in shards[1:]:
        factor_of = factor_of * one(*cut)
    return factor_of


def gaussian(key, shape, width, limit, cuts=(), kind=jnp.bfloat16):
    result = width * jax.random.normal(key, shape, jnp.float32)
    if cuts:
        result = result * shard_levels(key, shape, cuts, -0.22, 0.18)
    return jnp.clip(result, -limit, limit).astype(kind)


def setup_inputs(seed: int = 0) -> dict:
    seeds = jax.random.split(jax.random.key(seed), 4)
    activations = draw_activations(jax.random.fold_in(seeds[3], 71), 0)
    out_grads = draw_out_grads(jax.random.fold_in(seeds[3], 71), 0)
    weight = gaussian(seeds[2], (NBLOCKS, BLOCK, D), D ** -0.5, 0.09375, ((1, 4),))
    return dict(activations=activations, out_grads=out_grads, weight=weight)


DAMPING = 0.1
HIGH = lax.Precision.HIGHEST

def lowered(value):
    return lax.optimization_barrier(value.astype(jnp.bfloat16))

def batched(left, right):
    return jnp.einsum('kij,kjl->kil', left.astype(jnp.float32), right.astype(jnp.float32), precision=HIGH)

def reference(activations, out_grads, weight):
    sides = jnp.concatenate([activations, out_grads], axis=1)
    wide = sides.astype(jnp.float32)
    tokens = sides.shape[0]
    count = sides.shape[1]
    block = sides.shape[2]
    half = count // 2
    identity = jnp.eye(block, dtype=jnp.float32)[None]
    factor = jnp.einsum('tki,tkj->kij', wide, wide, precision=HIGH) / tokens + DAMPING * identity
    vector = jnp.ones((count, block), jnp.float32)
    image = vector
    for step in range(POWER):
        image = jnp.einsum('kij,kj->ki', factor, vector, precision=HIGH)
        if step + 1 < POWER:
            vector = image / jnp.sqrt(lax.optimization_barrier(jnp.sum(image * image, axis=1, keepdims=True)))
    scale = lax.optimization_barrier(jnp.sum(vector * image, axis=1)) / lax.optimization_barrier(jnp.sum(vector * vector, axis=1))
    start = factor / scale[:, None, None]
    start_low = lowered(start)
    first_low = lowered((3.0 * identity - start) / 2.0)
    square_low = lowered(batched(first_low, first_low))
    moved = batched(square_low, start_low)
    second_low = lowered((3.0 * identity - moved) / 2.0)
    roots = lowered(batched(first_low, second_low) / jnp.sqrt(scale)[:, None, None])
    whitened = lowered(jnp.einsum('tkj,kjc->tkc', wide, roots.astype(jnp.float32), precision=HIGH))
    acts_flat = whitened[:, :half, :].reshape(tokens, half * block).astype(jnp.float32)
    grads_low = whitened[:, half:, :].astype(jnp.float32)
    update = jnp.einsum('ta,tbc->abc', acts_flat, grads_low, precision=HIGH) / math.sqrt(tokens)
    grads_flat = out_grads.reshape(tokens, half * block).astype(jnp.float32)
    input_grad = jnp.einsum('tj,bcj->tbc', grads_flat, weight.astype(jnp.float32), precision=HIGH)
    return (update.astype(jnp.bfloat16), input_grad.astype(jnp.bfloat16))
```

```python
import math

import jax
import jax.numpy as jnp
from jax import lax
from jax.sharding import PartitionSpec as P

POWER = 3


DAMPING = 0.1
HIGH = lax.Precision.HIGHEST


def spread(piece):
    return lax.all_gather(piece, "out", axis=2, tiled=True)


def token_sums(maker, rows):
    return lax.psum_scatter(
        maker(jnp.int32(0), rows * lax.axis_size(("tok", "grp"))),
        ("tok", "grp"),
        scatter_dimension=0,
        tiled=True,
    )


def shared_rows(piece):
    return lax.all_gather(piece, ("tok", "grp"), axis=0, tiled=True)


def shared_total(vector):
    return lax.psum(vector, ("tok", "out", "grp"))


def diagonal_mask(rows, width, row_start, col_start):
    row_ids = row_start + lax.broadcasted_iota(jnp.int32, (rows, 1, width), 0)
    col_ids = col_start + lax.broadcasted_iota(jnp.int32, (rows, 1, width), 2)
    return jnp.where(row_ids == col_ids, 1.0, 0.0).astype(jnp.float32)


def multiply(left, right, gather_columns):
    row_band = spread(left)
    column_band = gather_columns(right)
    return jnp.einsum("rkj,jkc->rkc", row_band, column_band, preferred_element_type=jnp.float32)


def inverse_roots(tile, row_start, col_start, gather_columns, total):
    rows, count, width = tile.shape
    block = width * lax.axis_size("out")
    mask = diagonal_mask(rows, width, row_start, col_start)
    vector = jnp.ones((count, block), jnp.float32)
    image = vector
    for step in range(POWER):
        columns = lax.dynamic_slice_in_dim(vector, col_start, width, 1)
        part = jnp.einsum("rkc,kc->kr", tile, columns, precision=HIGH)
        placed = lax.dynamic_update_slice_in_dim(
            jnp.zeros((count, block), jnp.float32), part, row_start, 1
        )
        image = total(placed)
        if step + 1 < POWER:
            vector = image / jnp.sqrt(jnp.sum(image * image, axis=1, keepdims=True))
    scale = jnp.sum(vector * image, axis=1) / jnp.sum(vector * vector, axis=1)
    start = tile / scale[None, :, None]
    start_low = start.astype(jnp.bfloat16)
    first_low = ((3.0 * mask - start) / 2.0).astype(jnp.bfloat16)
    square_low = multiply(first_low, first_low, gather_columns).astype(jnp.bfloat16)
    moved = multiply(square_low, start_low, gather_columns)
    second_low = ((3.0 * mask - moved) / 2.0).astype(jnp.bfloat16)
    roots = multiply(first_low, second_low, gather_columns) / jnp.sqrt(scale)[None, :, None]
    return roots.astype(jnp.bfloat16)


def local(activations, out_grads, weight):
    tok_dev, blocks, width = activations.shape
    block = width * lax.axis_size("out")
    token_count = tok_dev * lax.axis_size("tok") * lax.axis_size("grp")
    col_start = lax.axis_index("out") * width
    local_sides = jnp.concatenate([activations, out_grads], axis=1)
    whole_sides = spread(local_sides)
    grads_whole = whole_sides[:, blocks:, :]
    weight_rows = weight.reshape(blocks, width, blocks, block)
    input_grad = jnp.einsum(
        "tjq,bcjq->tbc", grads_whole, weight_rows, preferred_element_type=jnp.float32
    ).astype(jnp.bfloat16)
    rows = block // (lax.axis_size("tok") * lax.axis_size("grp"))
    row_start = lax.axis_index(("tok", "grp")) * rows

    def shared_terms(start, span):
        return jnp.einsum(
            "tkr,tkc->rkc", whole_sides, local_sides, preferred_element_type=jnp.float32
        )

    sums = token_sums(shared_terms, rows)
    tile = sums / token_count + DAMPING * diagonal_mask(rows, width, row_start, col_start)
    roots = inverse_roots(tile, row_start, col_start, shared_rows, shared_total)
    bands = shared_rows(roots)
    whitened = jnp.einsum(
        "tkj,jkc->tkc", whole_sides, bands, preferred_element_type=jnp.float32
    ).astype(jnp.bfloat16)
    acts_whole = spread(whitened[:, :blocks, :]).reshape(tok_dev, blocks * block)
    grads_low = whitened[:, blocks:, :]
    owned_acts = lax.all_to_all(acts_whole, ("tok", "grp"), split_axis=1, concat_axis=0, tiled=True)
    update = jnp.einsum(
        "ta,tbc->abc",
        owned_acts,
        lax.all_gather(grads_low, ("tok", "grp"), axis=0, tiled=True),
        preferred_element_type=jnp.float32,
    )
    update = (update / math.sqrt(token_count)).astype(jnp.bfloat16)
    return (update, input_grad)


def token_space_whiten(sides, cols):
    tokens, block = sides.shape
    gram = jnp.einsum("tc,uc->tu", sides, sides, preferred_element_type=jnp.float32) / tokens
    ray_0 = jnp.sum(sides.astype(jnp.float32), axis=1)
    ray_1 = jnp.sum(gram * ray_0[None, :], axis=1) + DAMPING * ray_0
    ray_2 = jnp.sum(gram * ray_1[None, :], axis=1) + DAMPING * ray_1
    dots = [
        jnp.sum(ray_0 * ray_0),
        jnp.sum(ray_0 * ray_1),
        jnp.sum(ray_1 * ray_1),
        jnp.sum(ray_1 * ray_2),
        jnp.sum(ray_2 * ray_2),
    ]

    def moment(power):
        total = DAMPING**power * block
        for i in range(power):
            total = total + DAMPING ** (power - 1 - i) * dots[i] / tokens
        return total

    scale = moment(2 * POWER - 1) / moment(2 * POWER - 2)
    low = (gram / scale).astype(jnp.bfloat16)
    shift = DAMPING / scale

    def apply(value):
        product = jnp.einsum(
            "tu,uc->tc", low, value.astype(jnp.bfloat16), preferred_element_type=jnp.float32
        )
        return product + shift * value

    def first(value):
        return (3.0 * value - apply(value)) / 2.0

    head = first(cols.astype(jnp.float32))
    tail = first(first(apply(head)))
    return ((3.0 * head - tail) / 2.0 / jnp.sqrt(scale)).astype(jnp.bfloat16)


def planes(activations, out_grads, weight):
    tok_dev, blocks, width = activations.shape
    count = 2 * blocks
    tok, grp, out = (lax.axis_size(name) for name in ("tok", "grp", "out"))
    block = width * out
    token_count = tok_dev * tok * grp
    part = width // grp
    local_sides = jnp.concatenate([activations, out_grads], axis=1)
    pieces = jnp.swapaxes(local_sides, 0, 1)
    mine = lax.all_to_all(pieces, "tok", split_axis=0, concat_axis=0, tiled=True)
    mine = mine.reshape(tok * tok_dev, width)
    whole = lax.all_gather(mine, ("grp", "out"), axis=0, tiled=False)
    whole = whole.reshape(grp, out, tok * tok_dev, width)
    sides = jnp.transpose(whole, (0, 2, 1, 3)).reshape(token_count, block)
    start = lax.axis_index("out") * width + lax.axis_index("grp") * part
    cols = lax.dynamic_slice_in_dim(sides, start, part, 1)
    whitened = token_space_whiten(sides, cols)
    spread_low = lax.all_gather(whitened, ("tok", "grp"), axis=0, tiled=False)
    spread_low = spread_low.reshape(count, grp, token_count, part)
    grads_low = spread_low[blocks:]
    row = lax.axis_index(("tok", "grp"))
    own = lax.dynamic_index_in_dim(spread_low, row // out, 0, keepdims=False)
    owner = lax.rem(row, out) == lax.axis_index("out")
    acts_low = lax.psum(jnp.where(owner, own, jnp.zeros_like(own)), "out")
    update = jnp.einsum("yta,bxtc->yabxc", acts_low, grads_low, preferred_element_type=jnp.float32)
    update = (update / math.sqrt(token_count)).astype(jnp.bfloat16).reshape(width, blocks, width)
    grads_whole = spread(out_grads)
    weight_rows = weight.reshape(blocks, width, blocks, block)
    input_grad = jnp.einsum(
        "tjq,bcjq->tbc", grads_whole, weight_rows, preferred_element_type=jnp.float32
    ).astype(jnp.bfloat16)
    return (update, input_grad)


def solution(mesh):
    in_specs = (
        P(("tok", "grp"), None, "out"),
        P(("tok", "grp"), None, "out"),
        P(None, "out", None),
    )
    out_specs = (P(("tok", "grp"), None, "out"), P(("tok", "grp"), None, "out"))

    def body(activations, out_grads, weight):
        blocks = activations.shape[1]
        tok, grp, out = (mesh.shape[name] for name in ("tok", "grp", "out"))
        fits = tok == 2 * blocks and tok * grp == blocks * out
        return (planes if fits else local)(activations, out_grads, weight)

    return jax.shard_map(body, mesh=mesh, in_specs=in_specs, out_specs=out_specs, check_vma=False)
```

```python
import math

import jax
import jax.numpy as jnp
from jax import lax
from jax.experimental import pallas as pl
from jax.experimental.pallas import tpu as pltpu
from jax.sharding import PartitionSpec as P

POWER = 3


DAMPING = 0.1
HIGH = lax.Precision.HIGHEST


def spread(piece):
    return lax.all_gather(piece, "out", axis=2, tiled=True)


def token_sums(maker, rows):
    return lax.psum_scatter(
        maker(jnp.int32(0), rows * lax.axis_size(("tok", "grp"))),
        ("tok", "grp"),
        scatter_dimension=0,
        tiled=True,
    )


def shared_rows(piece):
    return lax.all_gather(piece, ("tok", "grp"), axis=0, tiled=True)


def shared_total(vector):
    return lax.psum(vector, ("tok", "out", "grp"))


def diagonal_mask(rows, width, row_start, col_start):
    row_ids = row_start + lax.broadcasted_iota(jnp.int32, (rows, 1, width), 0)
    col_ids = col_start + lax.broadcasted_iota(jnp.int32, (rows, 1, width), 2)
    return jnp.where(row_ids == col_ids, 1.0, 0.0).astype(jnp.float32)


def multiply(left, right, gather_columns):
    row_band = spread(left)
    column_band = gather_columns(right)
    return jnp.einsum("rkj,jkc->rkc", row_band, column_band, preferred_element_type=jnp.float32)


def inverse_roots(tile, row_start, col_start, gather_columns, total):
    rows, count, width = tile.shape
    block = width * lax.axis_size("out")
    mask = diagonal_mask(rows, width, row_start, col_start)
    vector = jnp.ones((count, block), jnp.float32)
    image = vector
    for step in range(POWER):
        columns = lax.dynamic_slice_in_dim(vector, col_start, width, 1)
        part = jnp.einsum("rkc,kc->kr", tile, columns, precision=HIGH)
        placed = lax.dynamic_update_slice_in_dim(
            jnp.zeros((count, block), jnp.float32), part, row_start, 1
        )
        image = total(placed)
        if step + 1 < POWER:
            vector = image / jnp.sqrt(jnp.sum(image * image, axis=1, keepdims=True))
    scale = jnp.sum(vector * image, axis=1) / jnp.sum(vector * vector, axis=1)
    start = tile / scale[None, :, None]
    start_low = start.astype(jnp.bfloat16)
    first_low = ((3.0 * mask - start) / 2.0).astype(jnp.bfloat16)
    square_low = multiply(first_low, first_low, gather_columns).astype(jnp.bfloat16)
    moved = multiply(square_low, start_low, gather_columns)
    second_low = ((3.0 * mask - moved) / 2.0).astype(jnp.bfloat16)
    roots = multiply(first_low, second_low, gather_columns) / jnp.sqrt(scale)[None, :, None]
    return roots.astype(jnp.bfloat16)


def local(activations, out_grads, weight):
    tok_dev, blocks, width = activations.shape
    block = width * lax.axis_size("out")
    token_count = tok_dev * lax.axis_size("tok") * lax.axis_size("grp")
    col_start = lax.axis_index("out") * width
    local_sides = jnp.concatenate([activations, out_grads], axis=1)
    whole_sides = spread(local_sides)
    grads_whole = whole_sides[:, blocks:, :]
    weight_rows = weight.reshape(blocks, width, blocks, block)
    input_grad = jnp.einsum(
        "tjq,bcjq->tbc", grads_whole, weight_rows, preferred_element_type=jnp.float32
    ).astype(jnp.bfloat16)
    rows = block // (lax.axis_size("tok") * lax.axis_size("grp"))
    row_start = lax.axis_index(("tok", "grp")) * rows

    def shared_terms(start, span):
        return jnp.einsum(
            "tkr,tkc->rkc", whole_sides, local_sides, preferred_element_type=jnp.float32
        )

    sums = token_sums(shared_terms, rows)
    tile = sums / token_count + DAMPING * diagonal_mask(rows, width, row_start, col_start)
    roots = inverse_roots(tile, row_start, col_start, shared_rows, shared_total)
    bands = shared_rows(roots)
    whitened = jnp.einsum(
        "tkj,jkc->tkc", whole_sides, bands, preferred_element_type=jnp.float32
    ).astype(jnp.bfloat16)
    acts_whole = spread(whitened[:, :blocks, :]).reshape(tok_dev, blocks * block)
    grads_low = whitened[:, blocks:, :]
    owned_acts = lax.all_to_all(acts_whole, ("tok", "grp"), split_axis=1, concat_axis=0, tiled=True)
    update = jnp.einsum(
        "ta,tbc->abc",
        owned_acts,
        lax.all_gather(grads_low, ("tok", "grp"), axis=0, tiled=True),
        preferred_element_type=jnp.float32,
    )
    update = (update / math.sqrt(token_count)).astype(jnp.bfloat16)
    return (update, input_grad)


MESH = pl.DeviceIdType.MESH
HOPS = (0, 1, 3, 2)
CHUNKS = 4


def greet(peers):
    barrier = pltpu.get_barrier_semaphore()
    for peer in peers:
        pl.semaphore_signal(barrier, inc=1, device_id=peer, device_id_type=MESH)
    pl.semaphore_wait(barrier, len(peers))


def remote(src, dst, send, recv, peer):
    return pltpu.make_async_remote_copy(
        src_ref=src, dst_ref=dst, send_sem=send, recv_sem=recv, device_id=peer, device_id_type=MESH
    )


def neighbours():
    z, o, y = lax.axis_index("tok"), lax.axis_index("out"), lax.axis_index("grp")
    ox = lax.rem(o + 2, 4)
    oc = o + 1 - 2 * lax.rem(o, 2)
    at = lambda a, b, c: {"tok": a, "out": b, "grp": c}
    zs = [lax.rem(z + j, 4) for j in range(4)]
    peers = [at(zs[j], o, y) for j in (1, 2, 3)]
    return z, o, y, ox, oc, zs, peers, at(z, o, 1 - y), at(z, ox, y), at(z, oc, y)


def collect_kernel(pieces, sides, grads, send, recv, grads_recv, local):
    z, o, y, ox, oc, zs, z_peers, y_peer, x_peer, c_peer = neighbours()
    rows, width = pieces.shape[1:]
    count = [0]

    def tile(oi, yi, zi):
        return sides.at[
            pl.ds(pl.multiple_of((yi * 4 + zi) * rows, rows), rows),
            pl.ds(pl.multiple_of(oi * width, width), width),
        ]

    def band(oi):
        return grads.at[:, :, pl.ds(pl.multiple_of(oi * width, width), width)]

    sent = []

    def push(src, dst, sem, peer):
        copy = remote(src, dst, send.at[count[0]], sem, peer)
        count[0] += 1
        copy.start()
        sent.append(copy)

    def sem_of(oi, yi, zi):
        return recv.at[oi * 8 + yi * 4 + zi]

    def arrived(oi, yi, zi):
        ref = tile(oi, yi, zi)
        remote(ref, ref, send.at[0], sem_of(oi, yi, zi), c_peer).wait_recv()
        return ref

    def forward(src, oi, yi, zi, peers):
        for peer in peers:
            push(src, tile(oi, yi, zi), sem_of(oi, yi, zi), peer)

    greet(z_peers + [y_peer, x_peer, c_peer])
    for j in (1, 3, 2):
        push(pieces.at[zs[j]], tile(o, y, z), sem_of(o, y, z), z_peers[j - 1])
    own = pltpu.make_async_copy(pieces.at[z], tile(o, y, z), local.at[0])
    own.start()
    forward(pieces.at[z], o, y, z, (y_peer, x_peer, c_peer))
    low = pieces.at[1:3]
    own_grads = pltpu.make_async_copy(low, band(o), local.at[1])
    own_grads.start()
    for peer in (x_peer, c_peer):
        push(low, band(o), grads_recv.at[o], peer)
    for j in (1, 3, 2):
        forward(arrived(o, y, zs[j]), o, y, zs[j], (y_peer, x_peer, c_peer))
    for step, j in enumerate(HOPS):
        ref = arrived(o, 1 - y, zs[j])
        forward(ref, o, 1 - y, zs[j], (x_peer, c_peer) if step % 2 == 0 else (c_peer,))
        ref = arrived(ox, y, zs[j])
        forward(ref, ox, y, zs[j], (y_peer, c_peer) if step % 2 == 1 else (c_peer,))
    ref = band(ox)
    remote(ref, ref, send.at[0], grads_recv.at[ox], c_peer).wait_recv()
    push(ref, ref, grads_recv.at[ox], c_peer)
    for j in HOPS:
        forward(arrived(ox, 1 - y, zs[j]), ox, 1 - y, zs[j], (c_peer,))
    oxc = lax.rem(oc + 2, 4)
    for oi in (oc, oxc):
        for yi in (y, 1 - y):
            for j in HOPS:
                arrived(oi, yi, zs[j])
        ref = band(oi)
        remote(ref, ref, send.at[0], grads_recv.at[oi], c_peer).wait_recv()
    own.wait()
    own_grads.wait()
    for copy in sent:
        copy.wait_send()


def collect(pieces):
    count, rows, width = pieces.shape
    sends = 3 + 3 * 4 + 3 * 4 + 4 + 3 + 4
    return pl.pallas_call(
        collect_kernel,
        out_shape=(
            jax.ShapeDtypeStruct((rows * 8, width * 4), pieces.dtype),
            jax.ShapeDtypeStruct((count // 2, rows, width * 4), pieces.dtype),
        ),
        in_specs=[pl.BlockSpec(memory_space=pltpu.VMEM)],
        out_specs=(pl.BlockSpec(memory_space=pltpu.VMEM), pl.BlockSpec(memory_space=pltpu.VMEM)),
        scratch_shapes=[
            pltpu.SemaphoreType.DMA((sends,)),
            pltpu.SemaphoreType.DMA((32,)),
            pltpu.SemaphoreType.DMA((4,)),
            pltpu.SemaphoreType.DMA((2,)),
        ],
        compiler_params=pltpu.CompilerParams(collective_id=0, has_side_effects=True),
        name="collect",
    )(pieces)


def deliver_kernel(low, grads, acts, g_send, y_send, g_recv, y_recv, a_send, a_recv, hub_send, hub_recv, local):
    z, o, y, ox, oc, zs, z_peers, y_peer, x_peer, c_peer = neighbours()
    tokens, part = low.shape
    rows = tokens // CHUNKS
    oxc = lax.rem(oc + 2, 4)
    row = 2 * z + y
    hub = lax.rem(row, 4)
    is_grad = (z == 1) | (z == 2)
    mine = z - 1
    base = (z // 3) * 2
    goal_z, goal_y = base + o // 2, lax.rem(o, 2)
    stays = (goal_z == z) & (goal_y == y)
    goal = {"tok": goal_z, "out": o, "grp": goal_y}
    source_z = (row // 4) * 3
    greet_all = z_peers + [y_peer, x_peer, c_peer] + [
        {"tok": zs[j], "out": o, "grp": 1 - y} for j in (1, 2, 3)
    ]
    greet(greet_all)

    def span(c):
        return pl.ds(c * rows, rows)

    def piece(c):
        return low.at[span(c), :]

    def half(yi):
        return pl.ds(pl.multiple_of(yi * part, part), part)

    def g_tile(b, yi, c):
        return grads.at[b, span(c), half(yi)]

    def a_tile(yi, c):
        return acts.at[span(c), half(yi)]

    def own_grad(c):
        return pltpu.make_async_copy(piece(c), g_tile(mine, y, c), local.at[c])

    def own_act(c):
        return pltpu.make_async_copy(piece(c), a_tile(y, c), local.at[c])

    def to_plane(c, j):
        return remote(
            piece(c), g_tile(mine, y, c), g_send.at[c * 3 + j - 1], g_recv.at[mine * CHUNKS + c], z_peers[j - 1]
        )

    def y_copy(src, b, c):
        return remote(
            src, g_tile(b, y, c), y_send.at[b * CHUNKS + c], y_recv.at[b * CHUNKS + c], y_peer
        )

    def to_hub(c):
        return remote(piece(c), a_tile(y, c), a_send.at[c], a_recv.at[y * CHUNKS + c], goal)

    def from_hub(yi, c, way, peer):
        ref = a_tile(yi, c)
        return remote(
            ref, ref, hub_send.at[way * 2 * CHUNKS + yi * CHUNKS + c], hub_recv.at[yi * CHUNKS + c], peer
        )

    for c in range(CHUNKS):

        @pl.when(is_grad)
        def _():
            for j in (1, 3, 2):
                to_plane(c, j).start()
            y_copy(piece(c), mine, c).start()
            own_grad(c).start()

        @pl.when(jnp.logical_not(is_grad) & stays)
        def _():
            own_act(c).start()

        @pl.when(jnp.logical_not(is_grad) & jnp.logical_not(stays))
        def _():
            to_hub(c).start()

    def hub_step(c):
        for yi in range(2):
            here = (source_z == z) & (y == yi)

            @pl.when((o == hub) & here)
            def _():
                own_act(c).wait()

            @pl.when((o == hub) & jnp.logical_not(here))
            def _():
                ref = a_tile(yi, c)
                remote(ref, ref, a_send.at[0], a_recv.at[yi * CHUNKS + c], c_peer).wait_recv()

            @pl.when(o == hub)
            def _():
                from_hub(yi, c, 0, x_peer).start()
                from_hub(yi, c, 1, c_peer).start()

    def relay_step(c):
        for yi in range(2):

            @pl.when(o != hub)
            def _():
                from_hub(yi, c, 0, c_peer).wait_recv()

            @pl.when(ox == hub)
            def _():
                from_hub(yi, c, 1, c_peer).start()

    for c in range(CHUNKS):
        for b in range(2):

            @pl.when(z != b + 1)
            def _():
                ref = g_tile(b, y, c)
                remote(ref, ref, g_send.at[0], g_recv.at[b * CHUNKS + c], c_peer).wait_recv()
                y_copy(ref, b, c).start()

        hub_step(c)
    for c in range(CHUNKS):
        relay_step(c)
    for c in range(CHUNKS):
        for b in range(2):
            ref = g_tile(b, 1 - y, c)
            remote(ref, ref, y_send.at[0], y_recv.at[b * CHUNKS + c], c_peer).wait_recv()
            y_copy(g_tile(b, y, c), b, c).wait_send()

        @pl.when(is_grad)
        def _():
            for j in (1, 3, 2):
                to_plane(c, j).wait_send()
            own_grad(c).wait()

        @pl.when(jnp.logical_not(is_grad) & jnp.logical_not(stays))
        def _():
            to_hub(c).wait_send()

        for yi in range(2):

            @pl.when(o == hub)
            def _():
                from_hub(yi, c, 0, x_peer).wait_send()

            @pl.when((o == hub) | (ox == hub))
            def _():
                from_hub(yi, c, 1, c_peer).wait_send()


def deliver(low):
    tokens, part = low.shape
    dma = pltpu.SemaphoreType.DMA
    return pl.pallas_call(
        deliver_kernel,
        out_shape=(
            jax.ShapeDtypeStruct((2, tokens, 2 * part), low.dtype),
            jax.ShapeDtypeStruct((tokens, 2 * part), low.dtype),
        ),
        in_specs=[pl.BlockSpec(memory_space=pltpu.VMEM)],
        out_specs=(pl.BlockSpec(memory_space=pltpu.VMEM), pl.BlockSpec(memory_space=pltpu.VMEM)),
        scratch_shapes=[
            dma((3 * CHUNKS,)),
            dma((2 * CHUNKS,)),
            dma((2 * CHUNKS,)),
            dma((2 * CHUNKS,)),
            dma((CHUNKS,)),
            dma((2 * CHUNKS,)),
            dma((4 * CHUNKS,)),
            dma((2 * CHUNKS,)),
            dma((CHUNKS,)),
        ],
        compiler_params=pltpu.CompilerParams(collective_id=1, has_side_effects=True),
        name="deliver",
    )(low)


def token_space_whiten(sides, cols):
    tokens, block = sides.shape
    gram = jnp.einsum("tc,uc->tu", sides, sides, preferred_element_type=jnp.float32) / tokens
    ray_0 = jnp.sum(sides.astype(jnp.float32), axis=1)
    ray_1 = jnp.sum(gram * ray_0[None, :], axis=1) + DAMPING * ray_0
    ray_2 = jnp.sum(gram * ray_1[None, :], axis=1) + DAMPING * ray_1
    dots = [
        jnp.sum(ray_0 * ray_0),
        jnp.sum(ray_0 * ray_1),
        jnp.sum(ray_1 * ray_1),
        jnp.sum(ray_1 * ray_2),
        jnp.sum(ray_2 * ray_2),
    ]

    def moment(power):
        total = DAMPING**power * block
        for i in range(power):
            total = total + DAMPING ** (power - 1 - i) * dots[i] / tokens
        return total

    scale = moment(2 * POWER - 1) / moment(2 * POWER - 2)
    low = (gram / scale).astype(jnp.bfloat16)
    shift = DAMPING / scale

    def apply(value):
        product = jnp.einsum(
            "tu,uc->tc", low, value.astype(jnp.bfloat16), preferred_element_type=jnp.float32
        )
        return product + shift * value

    def first(value):
        return (3.0 * value - apply(value)) / 2.0

    head = first(cols.astype(jnp.float32))
    tail = first(first(apply(head)))
    return ((3.0 * head - tail) / 2.0 / jnp.sqrt(scale)).astype(jnp.bfloat16)


def planes(activations, out_grads, weight):
    tok_dev, blocks, width = activations.shape
    block = width * lax.axis_size("out")
    part = width // lax.axis_size("grp")
    token_count = tok_dev * lax.axis_size(("tok", "grp"))
    pieces = jnp.stack([activations[:, 0], out_grads[:, 0], out_grads[:, 1], activations[:, 1]])
    sides, grads_whole = collect(pieces)
    start = lax.axis_index("out") * width + lax.axis_index("grp") * part
    cols = lax.dynamic_slice_in_dim(sides, start, part, 1)
    grads_low, acts_low = deliver(token_space_whiten(sides, cols))
    update = jnp.einsum("ta,btc->abc", acts_low, grads_low, preferred_element_type=jnp.float32)
    update = (update / math.sqrt(token_count)).astype(jnp.bfloat16)
    weight_rows = weight.reshape(blocks, width, blocks, block)
    input_grad = jnp.einsum(
        "jtq,bcjq->tbc", grads_whole, weight_rows, preferred_element_type=jnp.float32
    ).astype(jnp.bfloat16)
    return (update, input_grad)


def solution(mesh):
    in_specs = (
        P(("tok", "grp"), None, "out"),
        P(("tok", "grp"), None, "out"),
        P(None, "out", None),
    )
    out_specs = (P(("tok", "grp"), None, "out"), P(("tok", "grp"), None, "out"))

    def body(activations, out_grads, weight):
        blocks = activations.shape[1]
        tok, grp, out = (mesh.shape[name] for name in ("tok", "grp", "out"))
        fits = (blocks, tok, grp, out) == (2, 4, 2, 4)
        return (planes if fits else local)(activations, out_grads, weight)

    return jax.shard_map(body, mesh=mesh, in_specs=in_specs, out_specs=out_specs, check_vma=False)
```

```python
import math

import jax
import jax.numpy as jnp
from jax import lax
from jax.experimental import pallas as pl
from jax.experimental.pallas import tpu as pltpu
from jax.sharding import PartitionSpec as P

POWER = 3


DAMPING = 0.1
HIGH = lax.Precision.HIGHEST


def spread(piece):
    return lax.all_gather(piece, "out", axis=2, tiled=True)


def token_sums(maker, rows):
    return lax.psum_scatter(
        maker(jnp.int32(0), rows * lax.axis_size(("tok", "grp"))),
        ("tok", "grp"),
        scatter_dimension=0,
        tiled=True,
    )


def shared_rows(piece):
    return lax.all_gather(piece, ("tok", "grp"), axis=0, tiled=True)


def shared_total(vector):
    return lax.psum(vector, ("tok", "out", "grp"))


def diagonal_mask(rows, width, row_start, col_start):
    row_ids = row_start + lax.broadcasted_iota(jnp.int32, (rows, 1, width), 0)
    col_ids = col_start + lax.broadcasted_iota(jnp.int32, (rows, 1, width), 2)
    return jnp.where(row_ids == col_ids, 1.0, 0.0).astype(jnp.float32)


def multiply(left, right, gather_columns):
    row_band = spread(left)
    column_band = gather_columns(right)
    return jnp.einsum("rkj,jkc->rkc", row_band, column_band, preferred_element_type=jnp.float32)


def inverse_roots(tile, row_start, col_start, gather_columns, total):
    rows, count, width = tile.shape
    block = width * lax.axis_size("out")
    mask = diagonal_mask(rows, width, row_start, col_start)
    vector = jnp.ones((count, block), jnp.float32)
    image = vector
    for step in range(POWER):
        columns = lax.dynamic_slice_in_dim(vector, col_start, width, 1)
        part = jnp.einsum("rkc,kc->kr", tile, columns, precision=HIGH)
        placed = lax.dynamic_update_slice_in_dim(
            jnp.zeros((count, block), jnp.float32), part, row_start, 1
        )
        image = total(placed)
        if step + 1 < POWER:
            vector = image / jnp.sqrt(jnp.sum(image * image, axis=1, keepdims=True))
    scale = jnp.sum(vector * image, axis=1) / jnp.sum(vector * vector, axis=1)
    start = tile / scale[None, :, None]
    start_low = start.astype(jnp.bfloat16)
    first_low = ((3.0 * mask - start) / 2.0).astype(jnp.bfloat16)
    square_low = multiply(first_low, first_low, gather_columns).astype(jnp.bfloat16)
    moved = multiply(square_low, start_low, gather_columns)
    second_low = ((3.0 * mask - moved) / 2.0).astype(jnp.bfloat16)
    roots = multiply(first_low, second_low, gather_columns) / jnp.sqrt(scale)[None, :, None]
    return roots.astype(jnp.bfloat16)


def local(activations, out_grads, weight):
    tok_dev, blocks, width = activations.shape
    block = width * lax.axis_size("out")
    token_count = tok_dev * lax.axis_size("tok") * lax.axis_size("grp")
    col_start = lax.axis_index("out") * width
    local_sides = jnp.concatenate([activations, out_grads], axis=1)
    whole_sides = spread(local_sides)
    grads_whole = whole_sides[:, blocks:, :]
    weight_rows = weight.reshape(blocks, width, blocks, block)
    input_grad = jnp.einsum(
        "tjq,bcjq->tbc", grads_whole, weight_rows, preferred_element_type=jnp.float32
    ).astype(jnp.bfloat16)
    rows = block // (lax.axis_size("tok") * lax.axis_size("grp"))
    row_start = lax.axis_index(("tok", "grp")) * rows

    def shared_terms(start, span):
        return jnp.einsum(
            "tkr,tkc->rkc", whole_sides, local_sides, preferred_element_type=jnp.float32
        )

    sums = token_sums(shared_terms, rows)
    tile = sums / token_count + DAMPING * diagonal_mask(rows, width, row_start, col_start)
    roots = inverse_roots(tile, row_start, col_start, shared_rows, shared_total)
    bands = shared_rows(roots)
    whitened = jnp.einsum(
        "tkj,jkc->tkc", whole_sides, bands, preferred_element_type=jnp.float32
    ).astype(jnp.bfloat16)
    acts_whole = spread(whitened[:, :blocks, :]).reshape(tok_dev, blocks * block)
    grads_low = whitened[:, blocks:, :]
    owned_acts = lax.all_to_all(acts_whole, ("tok", "grp"), split_axis=1, concat_axis=0, tiled=True)
    update = jnp.einsum(
        "ta,tbc->abc",
        owned_acts,
        lax.all_gather(grads_low, ("tok", "grp"), axis=0, tiled=True),
        preferred_element_type=jnp.float32,
    )
    update = (update / math.sqrt(token_count)).astype(jnp.bfloat16)
    return (update, input_grad)


MESH = pl.DeviceIdType.MESH
HOPS = (0, 1, 3, 2)
CHUNKS = 4


def greet(peers):
    barrier = pltpu.get_barrier_semaphore()
    for peer in peers:
        pl.semaphore_signal(barrier, inc=1, device_id=peer, device_id_type=MESH)
    pl.semaphore_wait(barrier, len(peers))


def remote(src, dst, send, recv, peer):
    return pltpu.make_async_remote_copy(
        src_ref=src, dst_ref=dst, send_sem=send, recv_sem=recv, device_id=peer, device_id_type=MESH
    )


def held(z):
    return z + (z + 2) // 3 - 3 * (z // 3)


def neighbours():
    z, o, y = lax.axis_index("tok"), lax.axis_index("out"), lax.axis_index("grp")
    ox = lax.rem(o + 2, 4)
    oc = o + 1 - 2 * lax.rem(o, 2)
    at = lambda a, b, c: {"tok": a, "out": b, "grp": c}
    zs = [lax.rem(z + j, 4) for j in range(4)]
    peers = [at(zs[j], o, y) for j in (1, 2, 3)]
    return z, o, y, ox, oc, zs, peers, at(z, o, 1 - y), at(z, ox, y), at(z, oc, y)


def collect_kernel(pieces, sides, send, recv, local):
    z, o, y, ox, oc, zs, z_peers, y_peer, x_peer, c_peer = neighbours()
    rows, width = pieces.shape[1:]
    count = [0]

    def tile(oi, yi, zi):
        return sides.at[
            pl.ds(pl.multiple_of((yi * 4 + zi) * rows, rows), rows),
            pl.ds(pl.multiple_of(oi * width, width), width),
        ]

    sent = []

    def push(src, dst, sem, peer):
        copy = remote(src, dst, send.at[count[0]], sem, peer)
        count[0] += 1
        copy.start()
        sent.append(copy)

    def sem_of(oi, yi, zi):
        return recv.at[oi * 8 + yi * 4 + zi]

    def arrived(oi, yi, zi):
        ref = tile(oi, yi, zi)
        remote(ref, ref, send.at[0], sem_of(oi, yi, zi), c_peer).wait_recv()
        return ref

    def forward(src, oi, yi, zi, peers):
        for peer in peers:
            push(src, tile(oi, yi, zi), sem_of(oi, yi, zi), peer)

    greet(z_peers + [y_peer, x_peer, c_peer])
    for j in (1, 3, 2):
        push(pieces.at[held(zs[j])], tile(o, y, z), sem_of(o, y, z), z_peers[j - 1])
    own = pltpu.make_async_copy(pieces.at[held(z)], tile(o, y, z), local)
    own.start()
    forward(pieces.at[held(z)], o, y, z, (y_peer, x_peer, c_peer))
    for j in (1, 3, 2):
        forward(arrived(o, y, zs[j]), o, y, zs[j], (y_peer, x_peer, c_peer))
    for step, j in enumerate(HOPS):
        ref = arrived(o, 1 - y, zs[j])
        forward(ref, o, 1 - y, zs[j], (x_peer, c_peer) if step % 2 == 0 else (c_peer,))
        ref = arrived(ox, y, zs[j])
        forward(ref, ox, y, zs[j], (y_peer, c_peer) if step % 2 == 1 else (c_peer,))
    for j in HOPS:
        forward(arrived(ox, 1 - y, zs[j]), ox, 1 - y, zs[j], (c_peer,))
    oxc = lax.rem(oc + 2, 4)
    for oi in (oc, oxc):
        for yi in (y, 1 - y):
            for j in HOPS:
                arrived(oi, yi, zs[j])
    own.wait()
    for copy in sent:
        copy.wait_send()


def collect(pieces):
    _, rows, width = pieces.shape
    sends = 3 + 3 * 4 + 3 * 4 + 4
    return pl.pallas_call(
        collect_kernel,
        out_shape=jax.ShapeDtypeStruct((rows * 8, width * 4), pieces.dtype),
        in_specs=[pl.BlockSpec(memory_space=pltpu.VMEM)],
        out_specs=pl.BlockSpec(memory_space=pltpu.VMEM),
        scratch_shapes=[
            pltpu.SemaphoreType.DMA((sends,)),
            pltpu.SemaphoreType.DMA((32,)),
            pltpu.SemaphoreType.DMA,
        ],
        compiler_params=pltpu.CompilerParams(collective_id=0, has_side_effects=True),
        name="collect",
    )(pieces)


def deliver_kernel(low, pieces, grads, acts, raw, r_send, r_recv, g_send, y_send, g_recv, y_recv, a_send, a_recv, hub_send, hub_recv, local):
    z, o, y, ox, oc, zs, z_peers, y_peer, x_peer, c_peer = neighbours()
    tokens, part = low.shape
    rows = tokens // CHUNKS
    oxc = lax.rem(oc + 2, 4)
    row = 2 * z + y
    hub = lax.rem(row, 4)
    is_grad = (z == 1) | (z == 2)
    mine = z - 1
    base = (z // 3) * 2
    goal_z, goal_y = base + o // 2, lax.rem(o, 2)
    stays = (goal_z == z) & (goal_y == y)
    goal = {"tok": goal_z, "out": o, "grp": goal_y}
    source_z = (row // 4) * 3
    greet_all = z_peers + [y_peer, x_peer, c_peer] + [
        {"tok": zs[j], "out": o, "grp": 1 - y} for j in (1, 2, 3)
    ]
    greet(greet_all)
    width = pieces.shape[2]

    def band(oi):
        return raw.at[:, :, pl.ds(pl.multiple_of(oi * width, width), width)]

    own_raw = pieces.at[2:4]
    raw_local = pltpu.make_async_copy(own_raw, band(o), r_send.at[3])
    raw_x = remote(own_raw, band(o), r_send.at[0], r_recv.at[0], x_peer)
    raw_c = remote(own_raw, band(o), r_send.at[1], r_recv.at[1], c_peer)
    raw_xc = remote(band(ox), band(ox), r_send.at[2], r_recv.at[2], c_peer)
    raw_x.start()
    raw_c.start()
    raw_local.start()

    def span(c):
        return pl.ds(c * rows, rows)

    def piece(c):
        return low.at[span(c), :]

    def half(yi):
        return pl.ds(pl.multiple_of(yi * part, part), part)

    def g_tile(b, yi, c):
        return grads.at[b, span(c), half(yi)]

    def a_tile(yi, c):
        return acts.at[span(c), half(yi)]

    def own_grad(c):
        return pltpu.make_async_copy(piece(c), g_tile(mine, y, c), local.at[c])

    def own_act(c):
        return pltpu.make_async_copy(piece(c), a_tile(y, c), local.at[c])

    def to_plane(c, j):
        return remote(
            piece(c), g_tile(mine, y, c), g_send.at[c * 3 + j - 1], g_recv.at[mine * CHUNKS + c], z_peers[j - 1]
        )

    def y_copy(src, b, c):
        return remote(
            src, g_tile(b, y, c), y_send.at[b * CHUNKS + c], y_recv.at[b * CHUNKS + c], y_peer
        )

    def to_hub(c):
        return remote(piece(c), a_tile(y, c), a_send.at[c], a_recv.at[y * CHUNKS + c], goal)

    def from_hub(yi, c, way, peer):
        ref = a_tile(yi, c)
        return remote(
            ref, ref, hub_send.at[way * 2 * CHUNKS + yi * CHUNKS + c], hub_recv.at[yi * CHUNKS + c], peer
        )

    for c in range(CHUNKS):

        @pl.when(is_grad)
        def _():
            for j in (1, 3, 2):
                to_plane(c, j).start()
            y_copy(piece(c), mine, c).start()
            own_grad(c).start()

        @pl.when(jnp.logical_not(is_grad) & stays)
        def _():
            own_act(c).start()

        @pl.when(jnp.logical_not(is_grad) & jnp.logical_not(stays))
        def _():
            to_hub(c).start()

    def hub_step(c):
        for yi in range(2):
            here = (source_z == z) & (y == yi)

            @pl.when((o == hub) & here)
            def _():
                own_act(c).wait()

            @pl.when((o == hub) & jnp.logical_not(here))
            def _():
                ref = a_tile(yi, c)
                remote(ref, ref, a_send.at[0], a_recv.at[yi * CHUNKS + c], c_peer).wait_recv()

            @pl.when(o == hub)
            def _():
                from_hub(yi, c, 0, x_peer).start()
                from_hub(yi, c, 1, c_peer).start()

    def relay_step(c):
        for yi in range(2):

            @pl.when(o != hub)
            def _():
                from_hub(yi, c, 0, c_peer).wait_recv()

            @pl.when(ox == hub)
            def _():
                from_hub(yi, c, 1, c_peer).start()

    for c in range(CHUNKS):
        for b in range(2):

            @pl.when(z != b + 1)
            def _():
                ref = g_tile(b, y, c)
                remote(ref, ref, g_send.at[0], g_recv.at[b * CHUNKS + c], c_peer).wait_recv()
                y_copy(ref, b, c).start()

        hub_step(c)
    raw_x.wait_recv()
    raw_xc.start()
    for c in range(CHUNKS):
        relay_step(c)
    raw_c.wait_recv()
    raw_xc.wait()
    raw_x.wait_send()
    raw_c.wait_send()
    raw_local.wait()
    for c in range(CHUNKS):
        for b in range(2):
            ref = g_tile(b, 1 - y, c)
            remote(ref, ref, y_send.at[0], y_recv.at[b * CHUNKS + c], c_peer).wait_recv()
            y_copy(g_tile(b, y, c), b, c).wait_send()

        @pl.when(is_grad)
        def _():
            for j in (1, 3, 2):
                to_plane(c, j).wait_send()
            own_grad(c).wait()

        @pl.when(jnp.logical_not(is_grad) & jnp.logical_not(stays))
        def _():
            to_hub(c).wait_send()

        for yi in range(2):

            @pl.when(o == hub)
            def _():
                from_hub(yi, c, 0, x_peer).wait_send()

            @pl.when((o == hub) | (ox == hub))
            def _():
                from_hub(yi, c, 1, c_peer).wait_send()


def deliver(low, pieces):
    tokens, part = low.shape
    _, rows, width = pieces.shape
    dma = pltpu.SemaphoreType.DMA
    vmem = pl.BlockSpec(memory_space=pltpu.VMEM)
    return pl.pallas_call(
        deliver_kernel,
        out_shape=(
            jax.ShapeDtypeStruct((2, tokens, 2 * part), low.dtype),
            jax.ShapeDtypeStruct((tokens, 2 * part), low.dtype),
            jax.ShapeDtypeStruct((2, rows, 4 * width), low.dtype),
        ),
        in_specs=[vmem, vmem],
        out_specs=(vmem, vmem, vmem),
        scratch_shapes=[
            dma((4,)),
            dma((3,)),
            dma((3 * CHUNKS,)),
            dma((2 * CHUNKS,)),
            dma((2 * CHUNKS,)),
            dma((2 * CHUNKS,)),
            dma((CHUNKS,)),
            dma((2 * CHUNKS,)),
            dma((4 * CHUNKS,)),
            dma((2 * CHUNKS,)),
            dma((CHUNKS,)),
        ],
        compiler_params=pltpu.CompilerParams(collective_id=1, has_side_effects=True),
        name="deliver",
    )(low, pieces)


def whiten_kernel(sides, out, gram, low, ray, head, tail, left, right):
    tokens, block = sides.shape
    part = out.shape[1]
    tile = min(256, tokens)
    steps = tokens // tile
    across = (((1,), (1,)), ((), ()))
    ones = jnp.ones((8, block), sides.dtype)
    ray_0 = lax.dot_general(ones, sides[...], across, preferred_element_type=jnp.float32)[0:1]

    def span(i):
        return pl.ds(pl.multiple_of(i * tile, tile), tile)

    def gram_step(i, ray_2):
        product = lax.dot_general(
            sides[span(i), :], sides[...], across, preferred_element_type=jnp.float32
        )
        row_ids = i * tile + lax.broadcasted_iota(jnp.int32, (tile, tokens), 0)
        col_ids = lax.broadcasted_iota(jnp.int32, (tile, tokens), 1)
        product = product / tokens + jnp.where(row_ids == col_ids, DAMPING, 0.0)
        gram[span(i), :] = product
        column = jnp.sum(product * ray_0, axis=1, keepdims=True)
        ray[:, span(i)] = jnp.transpose(jnp.broadcast_to(column, (tile, 128)))[0:8]
        return ray_2 + jnp.sum(product * column, axis=0, keepdims=True)

    ray_2 = lax.fori_loop(0, steps, gram_step, jnp.zeros((1, tokens), jnp.float32))
    ray_1 = ray[0:1, :]

    def pair(a, b):
        return jnp.sum(a * b, axis=1, keepdims=True)

    dots = [
        pair(ray_0, ray_0),
        pair(ray_0, ray_1),
        pair(ray_1, ray_1),
        pair(ray_1, ray_2),
        pair(ray_2, ray_2),
    ]

    def moment(power):
        total = jnp.full((1, 1), DAMPING**power * block, jnp.float32)
        for i in range(power):
            total = total + DAMPING ** (power - 1 - i) * dots[i] / tokens
        return total

    scale = moment(2 * POWER - 1) / moment(2 * POWER - 2)
    inverse = 1.0 / scale
    root = 1.0 / jnp.sqrt(scale)
    start = lax.axis_index("out") * (2 * part) + lax.axis_index("grp") * part
    cols = pl.ds(pl.multiple_of(start, part), part)

    @pl.loop(0, steps)
    def _(i):
        low[span(i), :] = (gram[span(i), :] * inverse).astype(low.dtype)
        left[span(i), :] = sides[span(i), cols]

    def apply(i, source):
        return jnp.dot(low[span(i), :], source[...], preferred_element_type=jnp.float32)

    @pl.loop(0, steps)
    def _(i):
        value = sides[span(i), cols].astype(jnp.float32)
        value = 1.5 * value - 0.5 * apply(i, left)
        head[span(i), :] = value
        right[span(i), :] = value.astype(right.dtype)

    @pl.loop(0, steps)
    def _(i):
        value = apply(i, right)
        tail[span(i), :] = value
        left[span(i), :] = value.astype(left.dtype)

    @pl.loop(0, steps)
    def _(i):
        value = 1.5 * tail[span(i), :] - 0.5 * apply(i, left)
        tail[span(i), :] = value
        right[span(i), :] = value.astype(right.dtype)

    @pl.loop(0, steps)
    def _(i):
        value = 1.5 * tail[span(i), :] - 0.5 * apply(i, right)
        out[span(i), :] = ((1.5 * head[span(i), :] - 0.5 * value) * root).astype(out.dtype)


def whiten(sides, part):
    tokens, block = sides.shape
    return pl.pallas_call(
        whiten_kernel,
        out_shape=jax.ShapeDtypeStruct((tokens, part), sides.dtype),
        in_specs=[pl.BlockSpec(memory_space=pltpu.VMEM)],
        out_specs=pl.BlockSpec(memory_space=pltpu.VMEM),
        scratch_shapes=[
            pltpu.VMEM((tokens, tokens), jnp.float32),
            pltpu.VMEM((tokens, tokens), sides.dtype),
            pltpu.VMEM((8, tokens), jnp.float32),
            pltpu.VMEM((tokens, part), jnp.float32),
            pltpu.VMEM((tokens, part), jnp.float32),
            pltpu.VMEM((tokens, part), sides.dtype),
            pltpu.VMEM((tokens, part), sides.dtype),
        ],
        name="whiten",
    )(sides)


def planes(activations, out_grads, weight):
    tok_dev, blocks, width = activations.shape
    block = width * lax.axis_size("out")
    part = width // lax.axis_size("grp")
    token_count = tok_dev * lax.axis_size(("tok", "grp"))
    pieces = jnp.swapaxes(jnp.concatenate([activations, out_grads], axis=1), 0, 1)
    grads_low, acts_low, grads_whole = deliver(whiten(collect(pieces), part), pieces)
    update = jnp.einsum("ta,btc->abc", acts_low, grads_low, preferred_element_type=jnp.float32)
    update = (update / math.sqrt(token_count)).astype(jnp.bfloat16)
    weight_rows = weight.reshape(blocks, width, blocks, block)
    input_grad = jnp.einsum(
        "jtq,bcjq->tbc", grads_whole, weight_rows, preferred_element_type=jnp.float32
    ).astype(jnp.bfloat16)
    return (update, input_grad)


def solution(mesh):
    in_specs = (
        P(("tok", "grp"), None, "out"),
        P(("tok", "grp"), None, "out"),
        P(None, "out", None),
    )
    out_specs = (P(("tok", "grp"), None, "out"), P(("tok", "grp"), None, "out"))

    def body(activations, out_grads, weight):
        blocks = activations.shape[1]
        tok, grp, out = (mesh.shape[name] for name in ("tok", "grp", "out"))
        fits = (blocks, tok, grp, out) == (2, 4, 2, 4)
        return (planes if fits else local)(activations, out_grads, weight)

    return jax.shard_map(body, mesh=mesh, in_specs=in_specs, out_specs=out_specs, check_vma=False)
```

```python
import math

import jax
import jax.numpy as jnp
from jax import lax
from jax.experimental import pallas as pl
from jax.experimental.pallas import tpu as pltpu
from jax.sharding import PartitionSpec as P

POWER = 3


DAMPING = 0.1
HIGH = lax.Precision.HIGHEST


def spread(piece):
    return lax.all_gather(piece, "out", axis=2, tiled=True)


def token_sums(maker, rows):
    return lax.psum_scatter(
        maker(jnp.int32(0), rows * lax.axis_size(("tok", "grp"))),
        ("tok", "grp"),
        scatter_dimension=0,
        tiled=True,
    )


def shared_rows(piece):
    return lax.all_gather(piece, ("tok", "grp"), axis=0, tiled=True)


def shared_total(vector):
    return lax.psum(vector, ("tok", "out", "grp"))


def diagonal_mask(rows, width, row_start, col_start):
    row_ids = row_start + lax.broadcasted_iota(jnp.int32, (rows, 1, width), 0)
    col_ids = col_start + lax.broadcasted_iota(jnp.int32, (rows, 1, width), 2)
    return jnp.where(row_ids == col_ids, 1.0, 0.0).astype(jnp.float32)


def multiply(left, right, gather_columns):
    row_band = spread(left)
    column_band = gather_columns(right)
    return jnp.einsum("rkj,jkc->rkc", row_band, column_band, preferred_element_type=jnp.float32)


def inverse_roots(tile, row_start, col_start, gather_columns, total):
    rows, count, width = tile.shape
    block = width * lax.axis_size("out")
    mask = diagonal_mask(rows, width, row_start, col_start)
    vector = jnp.ones((count, block), jnp.float32)
    image = vector
    for step in range(POWER):
        columns = lax.dynamic_slice_in_dim(vector, col_start, width, 1)
        part = jnp.einsum("rkc,kc->kr", tile, columns, precision=HIGH)
        placed = lax.dynamic_update_slice_in_dim(
            jnp.zeros((count, block), jnp.float32), part, row_start, 1
        )
        image = total(placed)
        if step + 1 < POWER:
            vector = image / jnp.sqrt(jnp.sum(image * image, axis=1, keepdims=True))
    scale = jnp.sum(vector * image, axis=1) / jnp.sum(vector * vector, axis=1)
    start = tile / scale[None, :, None]
    start_low = start.astype(jnp.bfloat16)
    first_low = ((3.0 * mask - start) / 2.0).astype(jnp.bfloat16)
    square_low = multiply(first_low, first_low, gather_columns).astype(jnp.bfloat16)
    moved = multiply(square_low, start_low, gather_columns)
    second_low = ((3.0 * mask - moved) / 2.0).astype(jnp.bfloat16)
    roots = multiply(first_low, second_low, gather_columns) / jnp.sqrt(scale)[None, :, None]
    return roots.astype(jnp.bfloat16)


def local(activations, out_grads, weight):
    tok_dev, blocks, width = activations.shape
    block = width * lax.axis_size("out")
    token_count = tok_dev * lax.axis_size("tok") * lax.axis_size("grp")
    col_start = lax.axis_index("out") * width
    local_sides = jnp.concatenate([activations, out_grads], axis=1)
    whole_sides = spread(local_sides)
    grads_whole = whole_sides[:, blocks:, :]
    weight_rows = weight.reshape(blocks, width, blocks, block)
    input_grad = jnp.einsum(
        "tjq,bcjq->tbc", grads_whole, weight_rows, preferred_element_type=jnp.float32
    ).astype(jnp.bfloat16)
    rows = block // (lax.axis_size("tok") * lax.axis_size("grp"))
    row_start = lax.axis_index(("tok", "grp")) * rows

    def shared_terms(start, span):
        return jnp.einsum(
            "tkr,tkc->rkc", whole_sides, local_sides, preferred_element_type=jnp.float32
        )

    sums = token_sums(shared_terms, rows)
    tile = sums / token_count + DAMPING * diagonal_mask(rows, width, row_start, col_start)
    roots = inverse_roots(tile, row_start, col_start, shared_rows, shared_total)
    bands = shared_rows(roots)
    whitened = jnp.einsum(
        "tkj,jkc->tkc", whole_sides, bands, preferred_element_type=jnp.float32
    ).astype(jnp.bfloat16)
    acts_whole = spread(whitened[:, :blocks, :]).reshape(tok_dev, blocks * block)
    grads_low = whitened[:, blocks:, :]
    owned_acts = lax.all_to_all(acts_whole, ("tok", "grp"), split_axis=1, concat_axis=0, tiled=True)
    update = jnp.einsum(
        "ta,tbc->abc",
        owned_acts,
        lax.all_gather(grads_low, ("tok", "grp"), axis=0, tiled=True),
        preferred_element_type=jnp.float32,
    )
    update = (update / math.sqrt(token_count)).astype(jnp.bfloat16)
    return (update, input_grad)


MESH = pl.DeviceIdType.MESH
HOPS = (0, 1, 3, 2)
CHUNKS = 8
SPLIT = 2


def greet(peers):
    barrier = pltpu.get_barrier_semaphore()
    for peer in peers:
        pl.semaphore_signal(barrier, inc=1, device_id=peer, device_id_type=MESH)
    pl.semaphore_wait(barrier, len(peers))


def remote(src, dst, send, recv, peer):
    return pltpu.make_async_remote_copy(
        src_ref=src, dst_ref=dst, send_sem=send, recv_sem=recv, device_id=peer, device_id_type=MESH
    )


def held(z):
    return z + (z + 2) // 3 - 3 * (z // 3)


def neighbours():
    z, o, y = lax.axis_index("tok"), lax.axis_index("out"), lax.axis_index("grp")
    ox = lax.rem(o + 2, 4)
    oc = o + 1 - 2 * lax.rem(o, 2)
    at = lambda a, b, c: {"tok": a, "out": b, "grp": c}
    zs = [lax.rem(z + j, 4) for j in range(4)]
    peers = [at(zs[j], o, y) for j in (1, 2, 3)]
    return z, o, y, ox, oc, zs, peers, at(z, o, 1 - y), at(z, ox, y), at(z, oc, y)


def collect_kernel(pieces, sides, send, recv, local):
    z, o, y, ox, oc, zs, z_peers, y_peer, x_peer, c_peer = neighbours()
    width = pieces.shape[2]
    rows = pieces.shape[1] // SPLIT
    sent = []

    def tile(oi, yi, zi, s):
        return sides.at[
            pl.ds(pl.multiple_of(((yi * 4 + zi) * SPLIT + s) * rows, rows), rows),
            pl.ds(pl.multiple_of(oi * width, width), width),
        ]

    def piece(zi, s):
        return pieces.at[held(zi), pl.ds(s * rows, rows), :]

    def push(src, where, peer):
        copy = remote(src, tile(*where), send.at[len(sent)], sem_of(*where), peer)
        copy.start()
        sent.append(copy)

    def sem_of(oi, yi, zi, s):
        return recv.at[(oi * 8 + yi * 4 + zi) * SPLIT + s]

    def arrived(*where):
        ref = tile(*where)
        remote(ref, ref, send.at[0], sem_of(*where), c_peer).wait_recv()
        return ref

    def forward(src, where, peers):
        for peer in peers:
            push(src, where, peer)

    greet(z_peers + [y_peer, x_peer, c_peer])
    order = [(j, s) for j in HOPS for s in range(SPLIT)]
    owns = []
    for s in range(SPLIT):
        for j in (1, 3, 2):
            push(piece(zs[j], s), (o, y, z, s), z_peers[j - 1])
        forward(piece(z, s), (o, y, z, s), (y_peer, x_peer, c_peer))
        owns.append(pltpu.make_async_copy(piece(z, s), tile(o, y, z, s), local.at[s]))
        owns[-1].start()
    for j, s in order[SPLIT:]:
        where = (o, y, zs[j], s)
        forward(arrived(*where), where, (y_peer, x_peer, c_peer))
    for j, s in order:
        where = (o, 1 - y, zs[j], s)
        forward(arrived(*where), where, (x_peer, c_peer) if s % 2 == 0 else (c_peer,))
        where = (ox, y, zs[j], s)
        forward(arrived(*where), where, (y_peer, c_peer) if s % 2 == 1 else (c_peer,))
    for j, s in order:
        where = (ox, 1 - y, zs[j], s)
        forward(arrived(*where), where, (c_peer,))
    oxc = lax.rem(oc + 2, 4)
    for oi in (oc, oxc):
        for yi in (y, 1 - y):
            for j, s in order:
                arrived(oi, yi, zs[j], s)
    for copy in owns:
        copy.wait()
    for copy in sent:
        copy.wait_send()


def collect(pieces):
    _, rows, width = pieces.shape
    sends = (3 + 3 * 4 + 3 * 4 + 4) * SPLIT
    return pl.pallas_call(
        collect_kernel,
        out_shape=jax.ShapeDtypeStruct((rows * 8, width * 4), pieces.dtype),
        in_specs=[pl.BlockSpec(memory_space=pltpu.VMEM)],
        out_specs=pl.BlockSpec(memory_space=pltpu.VMEM),
        scratch_shapes=[
            pltpu.SemaphoreType.DMA((sends,)),
            pltpu.SemaphoreType.DMA((32 * SPLIT,)),
            pltpu.SemaphoreType.DMA((SPLIT,)),
        ],
        compiler_params=pltpu.CompilerParams(collective_id=0, has_side_effects=True),
        name="collect",
    )(pieces)


def deliver_kernel(
    low, pieces, weight, grads, acts, product,
    raw, held_weight, w_sem, r_send, r_recv, g_send, y_send, g_recv, y_recv,
    a_send, a_recv, x_send, c_send, c_recv, local,
):
    z, o, y, ox, oc, zs, z_peers, y_peer, x_peer, c_peer = neighbours()
    tokens, part = low.shape
    rows = tokens // CHUNKS
    width = pieces.shape[2]
    block = raw.shape[2]
    strip = width // 2
    is_grad = (z == 1) | (z == 2)
    is_act = jnp.logical_not(is_grad)
    mine = z - 1
    h = lax.rem(o, 2)
    goal_z = (z // 3) * 2 + o // 2
    stays = goal_z == z
    goal = {"tok": goal_z, "out": o, "grp": y}
    is_hub = o // 2 == lax.rem(z, 2)
    not_hub = jnp.logical_not(is_hub)
    here = is_act & stays
    greet(z_peers + [y_peer, x_peer, c_peer])

    def band(oi):
        return raw.at[:, :, pl.ds(pl.multiple_of(oi * width, width), width)]

    own_raw = pieces.at[2:4]
    raw_local = pltpu.make_async_copy(own_raw, band(o), r_send.at[3])
    raw_x = remote(own_raw, band(o), r_send.at[0], r_recv.at[0], x_peer)
    raw_c = remote(own_raw, band(o), r_send.at[1], r_recv.at[1], c_peer)
    raw_xc = remote(band(ox), band(ox), r_send.at[2], r_recv.at[2], c_peer)
    raw_x.start()
    raw_c.start()
    raw_local.start()

    def span(c):
        return pl.ds(c * rows, rows)

    def piece(c):
        return low.at[span(c), :]

    def half(i):
        return pl.ds(pl.multiple_of(i * part, part), part)

    def g_tile(b, yi, c):
        return grads.at[b, span(c), half(yi)]

    def a_tile(i, c):
        return acts.at[span(c), half(i)]

    def own_grad(c):
        return pltpu.make_async_copy(piece(c), g_tile(mine, y, c), local.at[c])

    def own_act(c):
        return pltpu.make_async_copy(piece(c), a_tile(h, c), local.at[c])

    def to_plane(c, j):
        return remote(
            piece(c), g_tile(mine, y, c), g_send.at[c * 3 + j - 1], g_recv.at[mine * CHUNKS + c], z_peers[j - 1]
        )

    def y_copy(src, b, c):
        return remote(src, g_tile(b, y, c), y_send.at[b * CHUNKS + c], y_recv.at[b * CHUNKS + c], y_peer)

    def to_hub(c):
        return remote(piece(c), a_tile(h, c), a_send.at[c], a_recv.at[c], goal)

    def over_x(c):
        return remote(a_tile(h, c), a_tile(h, c), x_send.at[c], a_recv.at[c], x_peer)

    def over_core(c):
        return remote(a_tile(h, c), a_tile(h, c), c_send.at[c], c_recv.at[c], c_peer)

    for c in range(CHUNKS):

        @pl.when(is_grad)
        def _():
            for j in (1, 3, 2):
                to_plane(c, j).start()
            y_copy(piece(c), mine, c).start()
            own_grad(c).start()

        @pl.when(here)
        def _():
            own_act(c).start()

        @pl.when(is_act & jnp.logical_not(stays))
        def _():
            to_hub(c).start()

    strips = [(b, i) for b in range(2) for i in range(2)]

    def load(n):
        b, i = strips[n]
        place = (b, pl.ds(i * strip, strip), slice(None))
        return pltpu.make_async_copy(weight.at[place], held_weight.at[place], w_sem.at[n])

    for n in range(4):
        load(n).start()

    def multiply(n):
        b, i = strips[n]
        load(n).wait()
        total = jnp.zeros((raw.shape[1], strip), jnp.float32)
        for k in range(2):
            total += lax.dot_general(
                raw[k],
                held_weight[b, pl.ds(i * strip, strip), pl.ds(k * block, block)],
                (((1,), (1,)), ((), ())),
                preferred_element_type=jnp.float32,
            )
        product[b, :, pl.ds(i * strip, strip)] = total.astype(product.dtype)

    def act_step(c, condition):
        @pl.when(condition & here)
        def _():
            own_act(c).wait()

        @pl.when(condition & jnp.logical_not(here))
        def _():
            over_x(c).wait_recv()

        @pl.when(condition & is_hub)
        def _():
            over_x(c).start()

        @pl.when(condition)
        def _():
            over_core(c).start()

    for c in range(CHUNKS):
        for b in range(2):

            @pl.when(z != b + 1)
            def _():
                ref = g_tile(b, y, c)
                remote(ref, ref, g_send.at[0], g_recv.at[b * CHUNKS + c], c_peer).wait_recv()
                y_copy(ref, b, c).start()

        act_step(c, is_hub)
        if c == 1:
            raw_x.wait_recv()
            raw_xc.start()
        if c == 2:
            raw_c.wait_recv()
            raw_xc.wait()
            raw_local.wait()
        if 2 <= c < 6:
            multiply(c - 2)
    for c in range(CHUNKS):
        act_step(c, not_hub)
    for c in range(CHUNKS):
        over_core(c).wait()
        for b in range(2):
            ref = g_tile(b, 1 - y, c)
            remote(ref, ref, y_send.at[0], y_recv.at[b * CHUNKS + c], c_peer).wait_recv()
            y_copy(g_tile(b, y, c), b, c).wait_send()

        @pl.when(is_grad)
        def _():
            for j in (1, 3, 2):
                to_plane(c, j).wait_send()
            own_grad(c).wait()

        @pl.when(is_act & jnp.logical_not(stays))
        def _():
            to_hub(c).wait_send()

        @pl.when(is_hub)
        def _():
            over_x(c).wait_send()

    raw_x.wait_send()
    raw_c.wait_send()


def deliver(low, pieces, weight):
    tokens, part = low.shape
    _, rows, width = pieces.shape
    dma = pltpu.SemaphoreType.DMA
    vmem = pl.BlockSpec(memory_space=pltpu.VMEM)
    return pl.pallas_call(
        deliver_kernel,
        out_shape=(
            jax.ShapeDtypeStruct((2, tokens, 2 * part), low.dtype),
            jax.ShapeDtypeStruct((tokens, 2 * part), low.dtype),
            jax.ShapeDtypeStruct((2, rows, width), low.dtype),
        ),
        in_specs=[vmem, vmem, pl.BlockSpec(memory_space=pl.ANY)],
        out_specs=(vmem, vmem, vmem),
        scratch_shapes=[
            pltpu.VMEM((2, rows, 4 * width), low.dtype),
            pltpu.VMEM(weight.shape, weight.dtype),
            dma((4,)),
            dma((4,)),
            dma((3,)),
            dma((3 * CHUNKS,)),
            dma((2 * CHUNKS,)),
            dma((2 * CHUNKS,)),
            dma((2 * CHUNKS,)),
            dma((CHUNKS,)),
            dma((CHUNKS,)),
            dma((CHUNKS,)),
            dma((CHUNKS,)),
            dma((CHUNKS,)),
            dma((CHUNKS,)),
        ],
        compiler_params=pltpu.CompilerParams(collective_id=1, has_side_effects=True),
        name="deliver",
    )(low, pieces, weight)


def whiten_kernel(sides, out, gram, low, ray, head, tail, left, right):
    tokens, block = sides.shape
    part = out.shape[1]
    tile = min(256, tokens)
    steps = tokens // tile
    across = (((1,), (1,)), ((), ()))
    ones = jnp.ones((8, block), sides.dtype)
    ray_0 = lax.dot_general(ones, sides[...], across, preferred_element_type=jnp.float32)[0:1]

    def span(i):
        return pl.ds(pl.multiple_of(i * tile, tile), tile)

    def gram_step(i, ray_2):
        product = lax.dot_general(
            sides[span(i), :], sides[...], across, preferred_element_type=jnp.float32
        )
        row_ids = i * tile + lax.broadcasted_iota(jnp.int32, (tile, tokens), 0)
        col_ids = lax.broadcasted_iota(jnp.int32, (tile, tokens), 1)
        product = product / tokens + jnp.where(row_ids == col_ids, DAMPING, 0.0)
        gram[span(i), :] = product
        column = jnp.sum(product * ray_0, axis=1, keepdims=True)
        ray[:, span(i)] = jnp.transpose(jnp.broadcast_to(column, (tile, 128)))[0:8]
        return ray_2 + jnp.sum(product * column, axis=0, keepdims=True)

    ray_2 = lax.fori_loop(0, steps, gram_step, jnp.zeros((1, tokens), jnp.float32))
    ray_1 = ray[0:1, :]

    def pair(a, b):
        return jnp.sum(a * b, axis=1, keepdims=True)

    dots = [
        pair(ray_0, ray_0),
        pair(ray_0, ray_1),
        pair(ray_1, ray_1),
        pair(ray_1, ray_2),
        pair(ray_2, ray_2),
    ]

    def moment(power):
        total = jnp.full((1, 1), DAMPING**power * block, jnp.float32)
        for i in range(power):
            total = total + DAMPING ** (power - 1 - i) * dots[i] / tokens
        return total

    scale = moment(2 * POWER - 1) / moment(2 * POWER - 2)
    inverse = 1.0 / scale
    root = 1.0 / jnp.sqrt(scale)
    z, o, y = lax.axis_index("tok"), lax.axis_index("out"), lax.axis_index("grp")
    act_start = 2 * (o // 2 * 2 + y) + lax.rem(o, 2)
    start = jnp.where((z == 1) | (z == 2), 2 * o + y, act_start) * part
    cols = pl.ds(pl.multiple_of(start, part), part)

    @pl.loop(0, steps)
    def _(i):
        low[span(i), :] = (gram[span(i), :] * inverse).astype(low.dtype)
        left[span(i), :] = sides[span(i), cols]

    def apply(i, source):
        return jnp.dot(low[span(i), :], source[...], preferred_element_type=jnp.float32)

    @pl.loop(0, steps)
    def _(i):
        value = sides[span(i), cols].astype(jnp.float32)
        value = 1.5 * value - 0.5 * apply(i, left)
        head[span(i), :] = value
        right[span(i), :] = value.astype(right.dtype)

    @pl.loop(0, steps)
    def _(i):
        value = apply(i, right)
        tail[span(i), :] = value
        left[span(i), :] = value.astype(left.dtype)

    @pl.loop(0, steps)
    def _(i):
        value = 1.5 * tail[span(i), :] - 0.5 * apply(i, left)
        tail[span(i), :] = value
        right[span(i), :] = value.astype(right.dtype)

    @pl.loop(0, steps)
    def _(i):
        value = 1.5 * tail[span(i), :] - 0.5 * apply(i, right)
        out[span(i), :] = ((1.5 * head[span(i), :] - 0.5 * value) * root).astype(out.dtype)


def whiten(sides, part):
    tokens, block = sides.shape
    return pl.pallas_call(
        whiten_kernel,
        out_shape=jax.ShapeDtypeStruct((tokens, part), sides.dtype),
        in_specs=[pl.BlockSpec(memory_space=pltpu.VMEM)],
        out_specs=pl.BlockSpec(memory_space=pltpu.VMEM),
        scratch_shapes=[
            pltpu.VMEM((tokens, tokens), jnp.float32),
            pltpu.VMEM((tokens, tokens), sides.dtype),
            pltpu.VMEM((8, tokens), jnp.float32),
            pltpu.VMEM((tokens, part), jnp.float32),
            pltpu.VMEM((tokens, part), jnp.float32),
            pltpu.VMEM((tokens, part), sides.dtype),
            pltpu.VMEM((tokens, part), sides.dtype),
        ],
        name="whiten",
    )(sides)


def planes(activations, out_grads, weight):
    tok_dev, _, width = activations.shape
    part = width // lax.axis_size("grp")
    token_count = tok_dev * lax.axis_size(("tok", "grp"))
    pieces = jnp.swapaxes(jnp.concatenate([activations, out_grads], axis=1), 0, 1)
    grads_low, acts_low, product = deliver(whiten(collect(pieces), part), pieces, weight)
    update = jnp.einsum("ta,btc->abc", acts_low, grads_low, preferred_element_type=jnp.float32)
    update = (update / math.sqrt(token_count)).astype(jnp.bfloat16)
    input_grad = jnp.swapaxes(product, 0, 1)
    return (update, input_grad)


def solution(mesh):
    in_specs = (
        P(("tok", "grp"), None, "out"),
        P(("tok", "grp"), None, "out"),
        P(None, "out", None),
    )
    out_specs = (P(("tok", "grp"), None, "out"), P(("tok", "grp"), None, "out"))

    def body(activations, out_grads, weight):
        blocks = activations.shape[1]
        tok, grp, out = (mesh.shape[name] for name in ("tok", "grp", "out"))
        fits = (blocks, tok, grp, out) == (2, 4, 2, 4)
        return (planes if fits else local)(activations, out_grads, weight)

    return jax.shard_map(body, mesh=mesh, in_specs=in_specs, out_specs=out_specs, check_vma=False)
```

```python
import math

import jax
import jax.numpy as jnp
from jax import lax
from jax.experimental import pallas as pl
from jax.experimental.pallas import tpu as pltpu
from jax.sharding import PartitionSpec as P

POWER = 3


DAMPING = 0.1
HIGH = lax.Precision.HIGHEST


def spread(piece):
    return lax.all_gather(piece, "out", axis=2, tiled=True)


def token_sums(maker, rows):
    return lax.psum_scatter(
        maker(jnp.int32(0), rows * lax.axis_size(("tok", "grp"))),
        ("tok", "grp"),
        scatter_dimension=0,
        tiled=True,
    )


def shared_rows(piece):
    return lax.all_gather(piece, ("tok", "grp"), axis=0, tiled=True)


def shared_total(vector):
    return lax.psum(vector, ("tok", "out", "grp"))


def diagonal_mask(rows, width, row_start, col_start):
    row_ids = row_start + lax.broadcasted_iota(jnp.int32, (rows, 1, width), 0)
    col_ids = col_start + lax.broadcasted_iota(jnp.int32, (rows, 1, width), 2)
    return jnp.where(row_ids == col_ids, 1.0, 0.0).astype(jnp.float32)


def multiply(left, right, gather_columns):
    row_band = spread(left)
    column_band = gather_columns(right)
    return jnp.einsum("rkj,jkc->rkc", row_band, column_band, preferred_element_type=jnp.float32)


def inverse_roots(tile, row_start, col_start, gather_columns, total):
    rows, count, width = tile.shape
    block = width * lax.axis_size("out")
    mask = diagonal_mask(rows, width, row_start, col_start)
    vector = jnp.ones((count, block), jnp.float32)
    image = vector
    for step in range(POWER):
        columns = lax.dynamic_slice_in_dim(vector, col_start, width, 1)
        part = jnp.einsum("rkc,kc->kr", tile, columns, precision=HIGH)
        placed = lax.dynamic_update_slice_in_dim(
            jnp.zeros((count, block), jnp.float32), part, row_start, 1
        )
        image = total(placed)
        if step + 1 < POWER:
            vector = image / jnp.sqrt(jnp.sum(image * image, axis=1, keepdims=True))
    scale = jnp.sum(vector * image, axis=1) / jnp.sum(vector * vector, axis=1)
    start = tile / scale[None, :, None]
    start_low = start.astype(jnp.bfloat16)
    first_low = ((3.0 * mask - start) / 2.0).astype(jnp.bfloat16)
    square_low = multiply(first_low, first_low, gather_columns).astype(jnp.bfloat16)
    moved = multiply(square_low, start_low, gather_columns)
    second_low = ((3.0 * mask - moved) / 2.0).astype(jnp.bfloat16)
    roots = multiply(first_low, second_low, gather_columns) / jnp.sqrt(scale)[None, :, None]
    return roots.astype(jnp.bfloat16)


def local(activations, out_grads, weight):
    tok_dev, blocks, width = activations.shape
    block = width * lax.axis_size("out")
    token_count = tok_dev * lax.axis_size("tok") * lax.axis_size("grp")
    col_start = lax.axis_index("out") * width
    local_sides = jnp.concatenate([activations, out_grads], axis=1)
    whole_sides = spread(local_sides)
    grads_whole = whole_sides[:, blocks:, :]
    weight_rows = weight.reshape(blocks, width, blocks, block)
    input_grad = jnp.einsum(
        "tjq,bcjq->tbc", grads_whole, weight_rows, preferred_element_type=jnp.float32
    ).astype(jnp.bfloat16)
    rows = block // (lax.axis_size("tok") * lax.axis_size("grp"))
    row_start = lax.axis_index(("tok", "grp")) * rows

    def shared_terms(start, span):
        return jnp.einsum(
            "tkr,tkc->rkc", whole_sides, local_sides, preferred_element_type=jnp.float32
        )

    sums = token_sums(shared_terms, rows)
    tile = sums / token_count + DAMPING * diagonal_mask(rows, width, row_start, col_start)
    roots = inverse_roots(tile, row_start, col_start, shared_rows, shared_total)
    bands = shared_rows(roots)
    whitened = jnp.einsum(
        "tkj,jkc->tkc", whole_sides, bands, preferred_element_type=jnp.float32
    ).astype(jnp.bfloat16)
    acts_whole = spread(whitened[:, :blocks, :]).reshape(tok_dev, blocks * block)
    grads_low = whitened[:, blocks:, :]
    owned_acts = lax.all_to_all(acts_whole, ("tok", "grp"), split_axis=1, concat_axis=0, tiled=True)
    update = jnp.einsum(
        "ta,tbc->abc",
        owned_acts,
        lax.all_gather(grads_low, ("tok", "grp"), axis=0, tiled=True),
        preferred_element_type=jnp.float32,
    )
    update = (update / math.sqrt(token_count)).astype(jnp.bfloat16)
    return (update, input_grad)


MESH = pl.DeviceIdType.MESH
HOPS = (0, 1, 3, 2)
CHUNKS = 8
SPLIT = 2


def greet(peers):
    barrier = pltpu.get_barrier_semaphore()
    for peer in peers:
        pl.semaphore_signal(barrier, inc=1, device_id=peer, device_id_type=MESH)
    pl.semaphore_wait(barrier, len(peers))


def remote(src, dst, send, recv, peer):
    return pltpu.make_async_remote_copy(
        src_ref=src, dst_ref=dst, send_sem=send, recv_sem=recv, device_id=peer, device_id_type=MESH
    )


def held(z):
    return z + 2 - 3 * ((z + 2) // 3) + z // 3


def neighbours():
    z, o, y = lax.axis_index("tok"), lax.axis_index("out"), lax.axis_index("grp")
    ox = lax.rem(o + 2, 4)
    oc = o + 1 - 2 * lax.rem(o, 2)
    at = lambda a, b, c: {"tok": a, "out": b, "grp": c}
    zs = [lax.rem(z + j, 4) for j in range(4)]
    peers = [at(zs[j], o, y) for j in (1, 2, 3)]
    return z, o, y, ox, oc, zs, peers, at(z, o, 1 - y), at(z, ox, y), at(z, oc, y)


def collect_kernel(pieces, sides, send, recv, local):
    z, o, y, ox, oc, zs, z_peers, y_peer, x_peer, c_peer = neighbours()
    width = pieces.shape[2]
    rows = pieces.shape[1] // SPLIT
    sent = []

    def tile(oi, yi, zi, s):
        return sides.at[
            pl.ds(pl.multiple_of(((yi * 4 + zi) * SPLIT + s) * rows, rows), rows),
            pl.ds(pl.multiple_of(oi * width, width), width),
        ]

    def piece(zi, s):
        return pieces.at[held(zi), pl.ds(s * rows, rows), :]

    def push(src, where, peer):
        copy = remote(src, tile(*where), send.at[len(sent)], sem_of(*where), peer)
        copy.start()
        sent.append(copy)

    def sem_of(oi, yi, zi, s):
        return recv.at[(oi * 8 + yi * 4 + zi) * SPLIT + s]

    def arrived(*where):
        ref = tile(*where)
        remote(ref, ref, send.at[0], sem_of(*where), c_peer).wait_recv()
        return ref

    def forward(src, where, peers):
        for peer in peers:
            push(src, where, peer)

    greet(z_peers + [y_peer, x_peer, c_peer])
    order = [(j, s) for j in HOPS for s in range(SPLIT)]
    owns = []
    for s in range(SPLIT):
        for j in (1, 3, 2):
            push(piece(zs[j], s), (o, y, z, s), z_peers[j - 1])
        forward(piece(z, s), (o, y, z, s), (y_peer, x_peer, c_peer))
        owns.append(pltpu.make_async_copy(piece(z, s), tile(o, y, z, s), local.at[s]))
        owns[-1].start()
    for j, s in order[SPLIT:]:
        where = (o, y, zs[j], s)
        forward(arrived(*where), where, (y_peer, x_peer, c_peer))
    for j, s in order:
        where = (o, 1 - y, zs[j], s)
        forward(arrived(*where), where, (x_peer, c_peer) if s % 2 == 0 else (c_peer,))
        where = (ox, y, zs[j], s)
        forward(arrived(*where), where, (y_peer, c_peer) if s % 2 == 1 else (c_peer,))
    for j, s in order:
        where = (ox, 1 - y, zs[j], s)
        forward(arrived(*where), where, (c_peer,))
    oxc = lax.rem(oc + 2, 4)
    for oi in (oc, oxc):
        for yi in (y, 1 - y):
            for j, s in order:
                arrived(oi, yi, zs[j], s)
    for copy in owns:
        copy.wait()
    for copy in sent:
        copy.wait_send()


def collect(pieces):
    _, rows, width = pieces.shape
    sends = (3 + 3 * 4 + 3 * 4 + 4) * SPLIT
    return pl.pallas_call(
        collect_kernel,
        out_shape=jax.ShapeDtypeStruct((rows * 8, width * 4), pieces.dtype),
        in_specs=[pl.BlockSpec(memory_space=pltpu.VMEM)],
        out_specs=pl.BlockSpec(memory_space=pltpu.VMEM),
        scratch_shapes=[
            pltpu.SemaphoreType.DMA((sends,)),
            pltpu.SemaphoreType.DMA((32 * SPLIT,)),
            pltpu.SemaphoreType.DMA((SPLIT,)),
        ],
        compiler_params=pltpu.CompilerParams(collective_id=0, has_side_effects=True),
        name="collect",
    )(pieces)


def deliver_kernel(
    low, pieces, weight, grads, acts, product,
    raw, held_weight, w_sem, r_send, r_recv, g_send, y_send, g_recv, y_recv,
    a_send, a_recv, x_send, x_recv, c_send, c_recv, local,
):
    z, o, y, ox, oc, zs, z_peers, y_peer, x_peer, c_peer = neighbours()
    tokens, part = low.shape
    rows = tokens // CHUNKS
    width = pieces.shape[2]
    block = raw.shape[2]
    strip = width // 2
    is_grad = (z == 0) | (z == 3)
    is_act = jnp.logical_not(is_grad)
    mine = z // 3
    h = o // 2
    goal_z = (z // 2) * 2 + lax.rem(o, 2)
    stays = goal_z == z
    goal = {"tok": goal_z, "out": o, "grp": y}
    onward = ({"tok": lax.rem(z + 1, 4), "out": o, "grp": y}, {"tok": lax.rem(z + 3, 4), "out": o, "grp": y})
    is_hub = lax.rem(o, 2) == lax.rem(z, 2)
    here = is_act & stays
    greet(z_peers + [y_peer, x_peer, c_peer])

    def band(oi):
        return raw.at[:, :, pl.ds(pl.multiple_of(oi * width, width), width)]

    own_raw = pieces.at[2:4]
    raw_local = pltpu.make_async_copy(own_raw, band(o), r_send.at[3])
    raw_x = remote(own_raw, band(o), r_send.at[0], r_recv.at[0], x_peer)
    raw_c = remote(own_raw, band(o), r_send.at[1], r_recv.at[1], c_peer)
    raw_xc = remote(band(ox), band(ox), r_send.at[2], r_recv.at[2], c_peer)
    raw_x.start()
    raw_c.start()
    raw_local.start()

    def span(c):
        return pl.ds(c * rows, rows)

    def piece(c):
        return low.at[span(c), :]

    def half(i):
        return pl.ds(pl.multiple_of(i * part, part), part)

    def g_tile(b, yi, c):
        return grads.at[b, span(c), half(yi)]

    def a_tile(i, c):
        return acts.at[span(c), half(i)]

    def own_grad(c):
        return pltpu.make_async_copy(piece(c), g_tile(mine, y, c), local.at[c])

    def own_act(c):
        return pltpu.make_async_copy(piece(c), a_tile(h, c), local.at[c])

    def to_plane(src, b, c):
        return remote(src, g_tile(b, y, c), g_send.at[b * CHUNKS + c], g_recv.at[b * CHUNKS + c], onward[b])

    def y_copy(src, b, c):
        return remote(src, g_tile(b, y, c), y_send.at[b * CHUNKS + c], y_recv.at[b * CHUNKS + c], y_peer)

    def to_hub(c):
        return remote(piece(c), a_tile(h, c), a_send.at[c], a_recv.at[c], goal)

    def over_x(c, i):
        return remote(a_tile(i, c), a_tile(i, c), x_send.at[c], x_recv.at[c], x_peer)

    def over_core(c, i):
        place = i * CHUNKS + c
        return remote(a_tile(i, c), a_tile(i, c), c_send.at[place], c_recv.at[place], c_peer)

    for c in range(CHUNKS):
        for b in range(2):

            @pl.when(z == 3 * b)
            def _():
                to_plane(piece(c), b, c).start()
                y_copy(piece(c), b, c).start()

        @pl.when(is_grad)
        def _():
            own_grad(c).start()

        @pl.when(here)
        def _():
            own_act(c).start()

        @pl.when(is_act & jnp.logical_not(stays))
        def _():
            to_hub(c).start()

    strips = [(b, i) for b in range(2) for i in range(2)]

    def load(n):
        b, i = strips[n]
        place = (b, pl.ds(i * strip, strip), slice(None))
        return pltpu.make_async_copy(weight.at[place], held_weight.at[place], w_sem.at[n])

    for n in range(4):
        load(n).start()

    def multiply(n):
        b, i = strips[n]
        load(n).wait()
        total = jnp.zeros((raw.shape[1], strip), jnp.float32)
        for k in range(2):
            total += lax.dot_general(
                raw[k],
                held_weight[b, pl.ds(i * strip, strip), pl.ds(k * block, block)],
                (((1,), (1,)), ((), ())),
                preferred_element_type=jnp.float32,
            )
        product[b, :, pl.ds(i * strip, strip)] = total.astype(product.dtype)

    def hub_step(c):
        @pl.when(here)
        def _():
            own_act(c).wait()

        @pl.when(is_hub & jnp.logical_not(here))
        def _():
            ref = a_tile(h, c)
            remote(ref, ref, a_send.at[0], a_recv.at[c], c_peer).wait_recv()

        @pl.when(is_hub)
        def _():
            over_x(c, h).start()
            over_core(c, h).start()

    def cross_step(c):
        @pl.when(is_hub)
        def _():
            over_x(c, 1 - h).wait_recv()
            over_core(c, 1 - h).start()

    for c in range(CHUNKS):
        for b in range(2):

            @pl.when(z != 3 * b)
            def _():
                ref = g_tile(b, y, c)
                remote(ref, ref, g_send.at[0], g_recv.at[b * CHUNKS + c], c_peer).wait_recv()

            @pl.when((z != 3 * b) & (z != 3 - 3 * b))
            def _():
                to_plane(g_tile(b, y, c), b, c).start()

            @pl.when(z != 3 * b)
            def _():
                y_copy(g_tile(b, y, c), b, c).start()

        hub_step(c)
        if c == 1:
            raw_x.wait_recv()
            raw_xc.start()
        if c == 2:
            raw_c.wait_recv()
            raw_xc.wait()
            raw_local.wait()
        if 2 <= c < 6:
            multiply(c - 2)
    for c in range(CHUNKS):
        cross_step(c)
    for c in range(CHUNKS):
        for b in range(2):
            ref = g_tile(b, 1 - y, c)
            remote(ref, ref, y_send.at[0], y_recv.at[b * CHUNKS + c], c_peer).wait_recv()
            y_copy(g_tile(b, y, c), b, c).wait_send()

            @pl.when(z != 3 - 3 * b)
            def _():
                to_plane(g_tile(b, y, c), b, c).wait_send()

        @pl.when(is_grad)
        def _():
            own_grad(c).wait()

        @pl.when(is_act & jnp.logical_not(stays))
        def _():
            to_hub(c).wait_send()

        for i in range(2):

            @pl.when(is_hub)
            def _():
                over_core(c, i).wait_send()

            @pl.when(jnp.logical_not(is_hub))
            def _():
                over_core(c, i).wait_recv()

        @pl.when(is_hub)
        def _():
            over_x(c, h).wait_send()

    raw_x.wait_send()
    raw_c.wait_send()


def deliver(low, pieces, weight):
    tokens, part = low.shape
    _, rows, width = pieces.shape
    dma = pltpu.SemaphoreType.DMA
    vmem = pl.BlockSpec(memory_space=pltpu.VMEM)
    return pl.pallas_call(
        deliver_kernel,
        out_shape=(
            jax.ShapeDtypeStruct((2, tokens, 2 * part), low.dtype),
            jax.ShapeDtypeStruct((tokens, 2 * part), low.dtype),
            jax.ShapeDtypeStruct((2, rows, width), low.dtype),
        ),
        in_specs=[vmem, vmem, pl.BlockSpec(memory_space=pl.ANY)],
        out_specs=(vmem, vmem, vmem),
        scratch_shapes=[
            pltpu.VMEM((2, rows, 4 * width), low.dtype),
            pltpu.VMEM(weight.shape, weight.dtype),
            dma((4,)),
            dma((4,)),
            dma((3,)),
            dma((2 * CHUNKS,)),
            dma((2 * CHUNKS,)),
            dma((2 * CHUNKS,)),
            dma((2 * CHUNKS,)),
            dma((CHUNKS,)),
            dma((CHUNKS,)),
            dma((CHUNKS,)),
            dma((CHUNKS,)),
            dma((2 * CHUNKS,)),
            dma((2 * CHUNKS,)),
            dma((CHUNKS,)),
        ],
        compiler_params=pltpu.CompilerParams(collective_id=1, has_side_effects=True),
        name="deliver",
    )(low, pieces, weight)


def whiten_kernel(sides, out, gram, low, ray, head, tail, left, right):
    tokens, block = sides.shape
    part = out.shape[1]
    tile = min(512, tokens)
    steps = tokens // tile
    across = (((1,), (1,)), ((), ()))
    ones = jnp.ones((8, block), sides.dtype)
    ray_0 = lax.dot_general(ones, sides[...], across, preferred_element_type=jnp.float32)[0:1]

    def span(i):
        return pl.ds(pl.multiple_of(i * tile, tile), tile)

    def gram_step(i, ray_2):
        product = lax.dot_general(
            sides[span(i), :], sides[...], across, preferred_element_type=jnp.float32
        )
        row_ids = i * tile + lax.broadcasted_iota(jnp.int32, (tile, tokens), 0)
        col_ids = lax.broadcasted_iota(jnp.int32, (tile, tokens), 1)
        product = product / tokens + jnp.where(row_ids == col_ids, DAMPING, 0.0)
        gram[span(i), :] = product
        column = jnp.sum(product * ray_0, axis=1, keepdims=True)
        ray[:, span(i)] = jnp.transpose(jnp.broadcast_to(column, (tile, 128)))[0:8]
        return ray_2 + jnp.sum(product * column, axis=0, keepdims=True)

    ray_2 = lax.fori_loop(0, steps, gram_step, jnp.zeros((1, tokens), jnp.float32))
    ray_1 = ray[0:1, :]

    def pair(a, b):
        return jnp.sum(a * b, axis=1, keepdims=True)

    dots = [
        pair(ray_0, ray_0),
        pair(ray_0, ray_1),
        pair(ray_1, ray_1),
        pair(ray_1, ray_2),
        pair(ray_2, ray_2),
    ]

    def moment(power):
        total = jnp.full((1, 1), DAMPING**power * block, jnp.float32)
        for i in range(power):
            total = total + DAMPING ** (power - 1 - i) * dots[i] / tokens
        return total

    scale = moment(2 * POWER - 1) / moment(2 * POWER - 2)
    inverse = 1.0 / scale
    root = 1.0 / jnp.sqrt(scale)
    z, o, y = lax.axis_index("tok"), lax.axis_index("out"), lax.axis_index("grp")
    act_start = 2 * (lax.rem(o, 2) * 2 + y) + o // 2
    start = jnp.where((z == 0) | (z == 3), 2 * o + y, act_start) * part
    cols = pl.ds(pl.multiple_of(start, part), part)

    @pl.loop(0, steps)
    def _(i):
        low[span(i), :] = (gram[span(i), :] * inverse).astype(low.dtype)
        left[span(i), :] = sides[span(i), cols]

    def apply(i, source):
        return jnp.dot(low[span(i), :], source[...], preferred_element_type=jnp.float32)

    @pl.loop(0, steps)
    def _(i):
        value = sides[span(i), cols].astype(jnp.float32)
        value = 1.5 * value - 0.5 * apply(i, left)
        head[span(i), :] = value
        right[span(i), :] = value.astype(right.dtype)

    @pl.loop(0, steps)
    def _(i):
        value = apply(i, right)
        tail[span(i), :] = value
        left[span(i), :] = value.astype(left.dtype)

    @pl.loop(0, steps)
    def _(i):
        value = 1.5 * tail[span(i), :] - 0.5 * apply(i, left)
        tail[span(i), :] = value
        right[span(i), :] = value.astype(right.dtype)

    @pl.loop(0, steps)
    def _(i):
        value = 1.5 * tail[span(i), :] - 0.5 * apply(i, right)
        out[span(i), :] = ((1.5 * head[span(i), :] - 0.5 * value) * root).astype(out.dtype)


def whiten(sides, part):
    tokens, block = sides.shape
    return pl.pallas_call(
        whiten_kernel,
        out_shape=jax.ShapeDtypeStruct((tokens, part), sides.dtype),
        in_specs=[pl.BlockSpec(memory_space=pltpu.VMEM)],
        out_specs=pl.BlockSpec(memory_space=pltpu.VMEM),
        scratch_shapes=[
            pltpu.VMEM((tokens, tokens), jnp.float32),
            pltpu.VMEM((tokens, tokens), sides.dtype),
            pltpu.VMEM((8, tokens), jnp.float32),
            pltpu.VMEM((tokens, part), jnp.float32),
            pltpu.VMEM((tokens, part), jnp.float32),
            pltpu.VMEM((tokens, part), sides.dtype),
            pltpu.VMEM((tokens, part), sides.dtype),
        ],
        name="whiten",
    )(sides)


def planes(activations, out_grads, weight):
    tok_dev, _, width = activations.shape
    part = width // lax.axis_size("grp")
    token_count = tok_dev * lax.axis_size(("tok", "grp"))
    pieces = jnp.swapaxes(jnp.concatenate([activations, out_grads], axis=1), 0, 1)
    grads_low, acts_low, product = deliver(whiten(collect(pieces), part), pieces, weight)
    update = jnp.einsum("ta,btc->abc", acts_low, grads_low, preferred_element_type=jnp.float32)
    update = (update / math.sqrt(token_count)).astype(jnp.bfloat16)
    input_grad = jnp.swapaxes(product, 0, 1)
    return (update, input_grad)


def solution(mesh):
    in_specs = (
        P(("tok", "grp"), None, "out"),
        P(("tok", "grp"), None, "out"),
        P(None, "out", None),
    )
    out_specs = (P(("tok", "grp"), None, "out"), P(("tok", "grp"), None, "out"))

    def body(activations, out_grads, weight):
        blocks = activations.shape[1]
        tok, grp, out = (mesh.shape[name] for name in ("tok", "grp", "out"))
        fits = (blocks, tok, grp, out) == (2, 4, 2, 4)
        return (planes if fits else local)(activations, out_grads, weight)

    return jax.shard_map(body, mesh=mesh, in_specs=in_specs, out_specs=out_specs, check_vma=False)
```

```python
import math

import jax
import jax.numpy as jnp
from jax import lax
from jax.experimental import pallas as pl
from jax.experimental.pallas import tpu as pltpu
from jax.sharding import PartitionSpec as P

POWER = 3


DAMPING = 0.1
HIGH = lax.Precision.HIGHEST


def spread(piece):
    return lax.all_gather(piece, "out", axis=2, tiled=True)


def token_sums(maker, rows):
    return lax.psum_scatter(
        maker(jnp.int32(0), rows * lax.axis_size(("tok", "grp"))),
        ("tok", "grp"),
        scatter_dimension=0,
        tiled=True,
    )


def shared_rows(piece):
    return lax.all_gather(piece, ("tok", "grp"), axis=0, tiled=True)


def shared_total(vector):
    return lax.psum(vector, ("tok", "out", "grp"))


def diagonal_mask(rows, width, row_start, col_start):
    row_ids = row_start + lax.broadcasted_iota(jnp.int32, (rows, 1, width), 0)
    col_ids = col_start + lax.broadcasted_iota(jnp.int32, (rows, 1, width), 2)
    return jnp.where(row_ids == col_ids, 1.0, 0.0).astype(jnp.float32)


def multiply(left, right, gather_columns):
    row_band = spread(left)
    column_band = gather_columns(right)
    return jnp.einsum("rkj,jkc->rkc", row_band, column_band, preferred_element_type=jnp.float32)


def inverse_roots(tile, row_start, col_start, gather_columns, total):
    rows, count, width = tile.shape
    block = width * lax.axis_size("out")
    mask = diagonal_mask(rows, width, row_start, col_start)
    vector = jnp.ones((count, block), jnp.float32)
    image = vector
    for step in range(POWER):
        columns = lax.dynamic_slice_in_dim(vector, col_start, width, 1)
        part = jnp.einsum("rkc,kc->kr", tile, columns, precision=HIGH)
        placed = lax.dynamic_update_slice_in_dim(
            jnp.zeros((count, block), jnp.float32), part, row_start, 1
        )
        image = total(placed)
        if step + 1 < POWER:
            vector = image / jnp.sqrt(jnp.sum(image * image, axis=1, keepdims=True))
    scale = jnp.sum(vector * image, axis=1) / jnp.sum(vector * vector, axis=1)
    start = tile / scale[None, :, None]
    start_low = start.astype(jnp.bfloat16)
    first_low = ((3.0 * mask - start) / 2.0).astype(jnp.bfloat16)
    square_low = multiply(first_low, first_low, gather_columns).astype(jnp.bfloat16)
    moved = multiply(square_low, start_low, gather_columns)
    second_low = ((3.0 * mask - moved) / 2.0).astype(jnp.bfloat16)
    roots = multiply(first_low, second_low, gather_columns) / jnp.sqrt(scale)[None, :, None]
    return roots.astype(jnp.bfloat16)


def local(activations, out_grads, weight):
    tok_dev, blocks, width = activations.shape
    block = width * lax.axis_size("out")
    token_count = tok_dev * lax.axis_size("tok") * lax.axis_size("grp")
    col_start = lax.axis_index("out") * width
    local_sides = jnp.concatenate([activations, out_grads], axis=1)
    whole_sides = spread(local_sides)
    grads_whole = whole_sides[:, blocks:, :]
    weight_rows = weight.reshape(blocks, width, blocks, block)
    input_grad = jnp.einsum(
        "tjq,bcjq->tbc", grads_whole, weight_rows, preferred_element_type=jnp.float32
    ).astype(jnp.bfloat16)
    rows = block // (lax.axis_size("tok") * lax.axis_size("grp"))
    row_start = lax.axis_index(("tok", "grp")) * rows

    def shared_terms(start, span):
        return jnp.einsum(
            "tkr,tkc->rkc", whole_sides, local_sides, preferred_element_type=jnp.float32
        )

    sums = token_sums(shared_terms, rows)
    tile = sums / token_count + DAMPING * diagonal_mask(rows, width, row_start, col_start)
    roots = inverse_roots(tile, row_start, col_start, shared_rows, shared_total)
    bands = shared_rows(roots)
    whitened = jnp.einsum(
        "tkj,jkc->tkc", whole_sides, bands, preferred_element_type=jnp.float32
    ).astype(jnp.bfloat16)
    acts_whole = spread(whitened[:, :blocks, :]).reshape(tok_dev, blocks * block)
    grads_low = whitened[:, blocks:, :]
    owned_acts = lax.all_to_all(acts_whole, ("tok", "grp"), split_axis=1, concat_axis=0, tiled=True)
    update = jnp.einsum(
        "ta,tbc->abc",
        owned_acts,
        lax.all_gather(grads_low, ("tok", "grp"), axis=0, tiled=True),
        preferred_element_type=jnp.float32,
    )
    update = (update / math.sqrt(token_count)).astype(jnp.bfloat16)
    return (update, input_grad)


MESH = pl.DeviceIdType.MESH
HOPS = (0, 1, 3, 2)
CHUNKS = 8
SPLIT = 2
LAG = 3


def greet(peers):
    barrier = pltpu.get_barrier_semaphore()
    for peer in peers:
        pl.semaphore_signal(barrier, inc=1, device_id=peer, device_id_type=MESH)
    pl.semaphore_wait(barrier, len(peers))


def remote(src, dst, send, recv, peer):
    return pltpu.make_async_remote_copy(
        src_ref=src, dst_ref=dst, send_sem=send, recv_sem=recv, device_id=peer, device_id_type=MESH
    )


def held(z):
    return z + 2 - 3 * ((z + 2) // 3) + z // 3


def neighbours():
    z, o, y = lax.axis_index("tok"), lax.axis_index("out"), lax.axis_index("grp")
    ox = lax.rem(o + 2, 4)
    oc = o + 1 - 2 * lax.rem(o, 2)
    at = lambda a, b, c: {"tok": a, "out": b, "grp": c}
    zs = [lax.rem(z + j, 4) for j in range(4)]
    peers = [at(zs[j], o, y) for j in (1, 2, 3)]
    return z, o, y, ox, oc, zs, peers, at(z, o, 1 - y), at(z, ox, y), at(z, oc, y)


def collect_kernel(pieces, sides, send, recv, local):
    z, o, y, ox, oc, zs, z_peers, y_peer, x_peer, c_peer = neighbours()
    width = pieces.shape[2]
    rows = pieces.shape[1] // SPLIT
    sent = []

    def tile(oi, yi, zi, s):
        return sides.at[
            pl.ds(pl.multiple_of(((yi * 4 + zi) * SPLIT + s) * rows, rows), rows),
            pl.ds(pl.multiple_of(oi * width, width), width),
        ]

    def piece(zi, s):
        return pieces.at[held(zi), pl.ds(s * rows, rows), :]

    def push(src, where, peer):
        copy = remote(src, tile(*where), send.at[len(sent)], sem_of(*where), peer)
        copy.start()
        sent.append(copy)

    def sem_of(oi, yi, zi, s):
        return recv.at[(oi * 8 + yi * 4 + zi) * SPLIT + s]

    def arrived(*where):
        ref = tile(*where)
        remote(ref, ref, send.at[0], sem_of(*where), c_peer).wait_recv()
        return ref

    def forward(src, where, peers):
        for peer in peers:
            push(src, where, peer)

    greet(z_peers + [y_peer, x_peer, c_peer])
    order = [(j, s) for j in HOPS for s in range(SPLIT)]
    owns = []
    for s in range(SPLIT):
        for j in (1, 3, 2):
            push(piece(zs[j], s), (o, y, z, s), z_peers[j - 1])
        forward(piece(z, s), (o, y, z, s), (y_peer, x_peer, c_peer))
        owns.append(pltpu.make_async_copy(piece(z, s), tile(o, y, z, s), local.at[s]))
        owns[-1].start()
    for j, s in order[SPLIT:]:
        where = (o, y, zs[j], s)
        forward(arrived(*where), where, (y_peer, x_peer, c_peer))
    for j, s in order:
        where = (o, 1 - y, zs[j], s)
        forward(arrived(*where), where, (x_peer, c_peer) if s % 2 == 0 else (c_peer,))
        where = (ox, y, zs[j], s)
        forward(arrived(*where), where, (y_peer, c_peer) if s % 2 == 1 else (c_peer,))
    for j, s in order:
        where = (ox, 1 - y, zs[j], s)
        forward(arrived(*where), where, (c_peer,))
    oxc = lax.rem(oc + 2, 4)
    for oi in (oc, oxc):
        for yi in (y, 1 - y):
            for j, s in order:
                arrived(oi, yi, zs[j], s)
    for copy in owns:
        copy.wait()
    for copy in sent:
        copy.wait_send()


def collect(pieces):
    _, rows, width = pieces.shape
    sends = (3 + 3 * 4 + 3 * 4 + 4) * SPLIT
    return pl.pallas_call(
        collect_kernel,
        out_shape=jax.ShapeDtypeStruct((rows * 8, width * 4), pieces.dtype),
        in_specs=[pl.BlockSpec(memory_space=pltpu.VMEM)],
        out_specs=pl.BlockSpec(memory_space=pltpu.VMEM),
        scratch_shapes=[
            pltpu.SemaphoreType.DMA((sends,)),
            pltpu.SemaphoreType.DMA((32 * SPLIT,)),
            pltpu.SemaphoreType.DMA((SPLIT,)),
        ],
        compiler_params=pltpu.CompilerParams(collective_id=0, has_side_effects=True),
        name="collect",
    )(pieces)


def deliver_kernel(
    low, pieces, weight, grads, acts, product,
    raw, held_weight, w_sem, r_send, r_recv, g_send, y_send, g_recv, y_recv,
    a_send, a_recv, x_send, x_recv, c_send, c_recv, local,
):
    z, o, y, ox, oc, zs, z_peers, y_peer, x_peer, c_peer = neighbours()
    tokens, part = low.shape
    rows = tokens // CHUNKS
    width = pieces.shape[2]
    block = raw.shape[2]
    strip = width // 2
    is_grad = (z == 0) | (z == 3)
    is_act = jnp.logical_not(is_grad)
    mine = z // 3
    h = o // 2
    goal_z = (z // 2) * 2 + lax.rem(o, 2)
    stays = goal_z == z
    goal = {"tok": goal_z, "out": o, "grp": y}
    near, far = z // 2, 1 - z // 2
    is_hub = lax.rem(o, 2) == lax.rem(z, 2)
    here = is_act & stays
    greet(z_peers + [y_peer, x_peer, c_peer])

    def band(oi):
        return raw.at[:, :, pl.ds(pl.multiple_of(oi * width, width), width)]

    own_raw = pieces.at[2:4]
    raw_local = pltpu.make_async_copy(own_raw, band(o), r_send.at[3])
    raw_x = remote(own_raw, band(o), r_send.at[0], r_recv.at[0], x_peer)
    raw_c = remote(own_raw, band(o), r_send.at[1], r_recv.at[1], c_peer)
    raw_xc = remote(band(ox), band(ox), r_send.at[2], r_recv.at[2], c_peer)
    raw_x.start()
    raw_c.start()
    raw_local.start()

    def span(c):
        return pl.ds(c * rows, rows)

    def piece(c):
        return low.at[span(c), :]

    def half(i):
        return pl.ds(pl.multiple_of(i * part, part), part)

    def g_tile(b, yi, c):
        return grads.at[b, span(c), half(yi)]

    def a_tile(i, c):
        return acts.at[span(c), half(i)]

    def own_grad(c):
        return pltpu.make_async_copy(piece(c), g_tile(mine, y, c), local.at[c])

    def own_act(c):
        return pltpu.make_async_copy(piece(c), a_tile(h, c), local.at[c])

    def to_plane(src, b, c):
        return remote(src, g_tile(b, y, c), g_send.at[b * CHUNKS + c], g_recv.at[b * CHUNKS + c], {"tok": lax.rem(z + 5 - 2 * b, 4), "out": o, "grp": y})

    def y_copy(src, b, c):
        return remote(src, g_tile(b, y, c), y_send.at[b * CHUNKS + c], y_recv.at[b * CHUNKS + c], y_peer)

    def to_hub(c):
        return remote(piece(c), a_tile(h, c), a_send.at[c], a_recv.at[c], goal)

    def over_x(c, i):
        return remote(a_tile(i, c), a_tile(i, c), x_send.at[c], x_recv.at[c], x_peer)

    def over_core(c, i):
        place = i * CHUNKS + c
        return remote(a_tile(i, c), a_tile(i, c), c_send.at[place], c_recv.at[place], c_peer)

    for c in range(CHUNKS):
        for b in range(2):

            @pl.when(z == 3 * b)
            def _():
                to_plane(piece(c), b, c).start()
                y_copy(piece(c), b, c).start()

        @pl.when(is_grad)
        def _():
            own_grad(c).start()

        @pl.when(here)
        def _():
            own_act(c).start()

        @pl.when(is_act & jnp.logical_not(stays))
        def _():
            to_hub(c).start()

    strips = [(b, i) for b in range(2) for i in range(2)]

    def load(n):
        b, i = strips[n]
        place = (b, pl.ds(i * strip, strip), slice(None))
        return pltpu.make_async_copy(weight.at[place], held_weight.at[place], w_sem.at[n])

    for n in range(4):
        load(n).start()

    def multiply(n):
        b, i = strips[n]
        load(n).wait()
        total = jnp.zeros((raw.shape[1], strip), jnp.float32)
        for k in range(2):
            total += lax.dot_general(
                raw[k],
                held_weight[b, pl.ds(i * strip, strip), pl.ds(k * block, block)],
                (((1,), (1,)), ((), ())),
                preferred_element_type=jnp.float32,
            )
        product[b, :, pl.ds(i * strip, strip)] = total.astype(product.dtype)

    def hub_step(c):
        @pl.when(here)
        def _():
            own_act(c).wait()

        @pl.when(is_hub & jnp.logical_not(here))
        def _():
            ref = a_tile(h, c)
            remote(ref, ref, a_send.at[0], a_recv.at[c], c_peer).wait_recv()

        @pl.when(is_hub)
        def _():
            over_x(c, h).start()
            over_core(c, h).start()

    def cross_step(c):
        @pl.when(is_hub)
        def _():
            over_x(c, 1 - h).wait_recv()
            over_core(c, 1 - h).start()

    def take(b, c):
        ref = g_tile(b, y, c)
        remote(ref, ref, g_send.at[0], g_recv.at[b * CHUNKS + c], c_peer).wait_recv()

        @pl.when(is_act)
        def _():
            to_plane(ref, b, c).start()

        y_copy(ref, b, c).start()

    for step in range(CHUNKS + LAG):
        if step < CHUNKS:

            @pl.when(is_act)
            def _():
                take(near, step)

            hub_step(step)
        if step >= LAG:
            take(far, step - LAG)
        if step == 1:
            raw_x.wait_recv()
            raw_xc.start()
        if step == 2:
            raw_c.wait_recv()
            raw_xc.wait()
            raw_local.wait()
        if 3 <= step < 7:
            multiply(step - 3)
    for c in range(CHUNKS):
        cross_step(c)
    for c in range(CHUNKS):
        for b in range(2):
            ref = g_tile(b, 1 - y, c)
            remote(ref, ref, y_send.at[0], y_recv.at[b * CHUNKS + c], c_peer).wait_recv()
            y_copy(g_tile(b, y, c), b, c).wait_send()

            @pl.when(z != 3 - 3 * b)
            def _():
                to_plane(g_tile(b, y, c), b, c).wait_send()

        @pl.when(is_grad)
        def _():
            own_grad(c).wait()

        @pl.when(is_act & jnp.logical_not(stays))
        def _():
            to_hub(c).wait_send()

        for i in range(2):

            @pl.when(is_hub)
            def _():
                over_core(c, i).wait_send()

            @pl.when(jnp.logical_not(is_hub))
            def _():
                over_core(c, i).wait_recv()

        @pl.when(is_hub)
        def _():
            over_x(c, h).wait_send()

    raw_x.wait_send()
    raw_c.wait_send()


def deliver(low, pieces, weight):
    tokens, part = low.shape
    _, rows, width = pieces.shape
    dma = pltpu.SemaphoreType.DMA
    vmem = pl.BlockSpec(memory_space=pltpu.VMEM)
    return pl.pallas_call(
        deliver_kernel,
        out_shape=(
            jax.ShapeDtypeStruct((2, tokens, 2 * part), low.dtype),
            jax.ShapeDtypeStruct((tokens, 2 * part), low.dtype),
            jax.ShapeDtypeStruct((2, rows, width), low.dtype),
        ),
        in_specs=[vmem, vmem, pl.BlockSpec(memory_space=pl.ANY)],
        out_specs=(vmem, vmem, vmem),
        scratch_shapes=[
            pltpu.VMEM((2, rows, 4 * width), low.dtype),
            pltpu.VMEM(weight.shape, weight.dtype),
            dma((4,)),
            dma((4,)),
            dma((3,)),
            dma((2 * CHUNKS,)),
            dma((2 * CHUNKS,)),
            dma((2 * CHUNKS,)),
            dma((2 * CHUNKS,)),
            dma((CHUNKS,)),
            dma((CHUNKS,)),
            dma((CHUNKS,)),
            dma((CHUNKS,)),
            dma((2 * CHUNKS,)),
            dma((2 * CHUNKS,)),
            dma((CHUNKS,)),
        ],
        compiler_params=pltpu.CompilerParams(collective_id=1, has_side_effects=True),
        name="deliver",
    )(low, pieces, weight)


def whiten_kernel(sides, out, gram, low, ray, head, tail, left, right):
    tokens, block = sides.shape
    part = out.shape[1]
    tile = min(512, tokens)
    steps = tokens // tile
    across = (((1,), (1,)), ((), ()))
    ones = jnp.ones((8, block), sides.dtype)
    ray_0 = lax.dot_general(ones, sides[...], across, preferred_element_type=jnp.float32)[0:1]

    def span(i):
        return pl.ds(pl.multiple_of(i * tile, tile), tile)

    def gram_step(i, ray_2):
        product = lax.dot_general(
            sides[span(i), :], sides[...], across, preferred_element_type=jnp.float32
        )
        row_ids = i * tile + lax.broadcasted_iota(jnp.int32, (tile, tokens), 0)
        col_ids = lax.broadcasted_iota(jnp.int32, (tile, tokens), 1)
        product = product / tokens + jnp.where(row_ids == col_ids, DAMPING, 0.0)
        gram[span(i), :] = product
        column = jnp.sum(product * ray_0, axis=1, keepdims=True)
        ray[:, span(i)] = jnp.transpose(jnp.broadcast_to(column, (tile, 128)))[0:8]
        return ray_2 + jnp.sum(product * column, axis=0, keepdims=True)

    ray_2 = lax.fori_loop(0, steps, gram_step, jnp.zeros((1, tokens), jnp.float32))
    ray_1 = ray[0:1, :]

    def pair(a, b):
        return jnp.sum(a * b, axis=1, keepdims=True)

    dots = [
        pair(ray_0, ray_0),
        pair(ray_0, ray_1),
        pair(ray_1, ray_1),
        pair(ray_1, ray_2),
        pair(ray_2, ray_2),
    ]

    def moment(power):
        total = jnp.full((1, 1), DAMPING**power * block, jnp.float32)
        for i in range(power):
            total = total + DAMPING ** (power - 1 - i) * dots[i] / tokens
        return total

    scale = moment(2 * POWER - 1) / moment(2 * POWER - 2)
    inverse = 1.0 / scale
    root = 1.0 / jnp.sqrt(scale)
    z, o, y = lax.axis_index("tok"), lax.axis_index("out"), lax.axis_index("grp")
    act_start = 2 * (lax.rem(o, 2) * 2 + y) + o // 2
    start = jnp.where((z == 0) | (z == 3), 2 * o + y, act_start) * part
    cols = pl.ds(pl.multiple_of(start, part), part)

    @pl.loop(0, steps)
    def _(i):
        low[span(i), :] = (gram[span(i), :] * inverse).astype(low.dtype)
        left[span(i), :] = sides[span(i), cols]

    def apply(i, source):
        return jnp.dot(low[span(i), :], source[...], preferred_element_type=jnp.float32)

    @pl.loop(0, steps)
    def _(i):
        value = sides[span(i), cols].astype(jnp.float32)
        value = 1.5 * value - 0.5 * apply(i, left)
        head[span(i), :] = value
        right[span(i), :] = value.astype(right.dtype)

    @pl.loop(0, steps)
    def _(i):
        value = apply(i, right)
        tail[span(i), :] = value
        left[span(i), :] = value.astype(left.dtype)

    @pl.loop(0, steps)
    def _(i):
        value = 1.5 * tail[span(i), :] - 0.5 * apply(i, left)
        tail[span(i), :] = value
        right[span(i), :] = value.astype(right.dtype)

    @pl.loop(0, steps)
    def _(i):
        value = 1.5 * tail[span(i), :] - 0.5 * apply(i, right)
        out[span(i), :] = ((1.5 * head[span(i), :] - 0.5 * value) * root).astype(out.dtype)


def whiten(sides, part):
    tokens, block = sides.shape
    return pl.pallas_call(
        whiten_kernel,
        out_shape=jax.ShapeDtypeStruct((tokens, part), sides.dtype),
        in_specs=[pl.BlockSpec(memory_space=pltpu.VMEM)],
        out_specs=pl.BlockSpec(memory_space=pltpu.VMEM),
        scratch_shapes=[
            pltpu.VMEM((tokens, tokens), jnp.float32),
            pltpu.VMEM((tokens, tokens), sides.dtype),
            pltpu.VMEM((8, tokens), jnp.float32),
            pltpu.VMEM((tokens, part), jnp.float32),
            pltpu.VMEM((tokens, part), jnp.float32),
            pltpu.VMEM((tokens, part), sides.dtype),
            pltpu.VMEM((tokens, part), sides.dtype),
        ],
        name="whiten",
    )(sides)


def planes(activations, out_grads, weight):
    tok_dev, _, width = activations.shape
    part = width // lax.axis_size("grp")
    token_count = tok_dev * lax.axis_size(("tok", "grp"))
    pieces = jnp.swapaxes(jnp.concatenate([activations, out_grads], axis=1), 0, 1)
    grads_low, acts_low, product = deliver(whiten(collect(pieces), part), pieces, weight)
    update = jnp.einsum("ta,btc->abc", acts_low, grads_low, preferred_element_type=jnp.float32)
    update = (update / math.sqrt(token_count)).astype(jnp.bfloat16)
    input_grad = jnp.swapaxes(product, 0, 1)
    return (update, input_grad)


def solution(mesh):
    in_specs = (
        P(("tok", "grp"), None, "out"),
        P(("tok", "grp"), None, "out"),
        P(None, "out", None),
    )
    out_specs = (P(("tok", "grp"), None, "out"), P(("tok", "grp"), None, "out"))

    def body(activations, out_grads, weight):
        blocks = activations.shape[1]
        tok, grp, out = (mesh.shape[name] for name in ("tok", "grp", "out"))
        fits = (blocks, tok, grp, out) == (2, 4, 2, 4)
        return (planes if fits else local)(activations, out_grads, weight)

    return jax.shard_map(body, mesh=mesh, in_specs=in_specs, out_specs=out_specs, check_vma=False)
```
